32 devices in a mesh: row: 4 (over x, core), col: 2 (over y), depth: 4 (over z).
Axes of the slice: x: 2, y: 2, z: 4, core: 2. Of those that a mesh axis runs over, the one named last changes fastest.
Arguments:
- diag_two: float32 [256, 256], replicated, may hold values from -3 to 3, as said below
- diag_one: float32 [256, 256], replicated, may hold values from -3 to 3, as said below
- cross_tile: float32 [256, 256], replicated, may hold values from -0.375 to 0.375
- left_two: float32 [256, 4096], P(None, ('col', 'depth')), may hold values from -0.375 to 0.375
- left_one: float32 [256, 4096], P(None, ('col', 'depth')), may hold values from -0.375 to 0.375
- below_left: float32 [4096, 4096], P('row', ('col', 'depth')), may hold values from -0.09375 to 0.09375
- panel_two: float32 [4096, 256], P('row', 'col'), may hold values from -0.09375 to 0.09375
- panel_one: float32 [4096, 256], P('row', 'col'), may hold values from -0.09375 to 0.09375
- grad_diag_two: float32 [256, 256], replicated, may hold values from -6 to 6
- grad_diag_one: float32 [256, 256], replicated, may hold values from -6 to 6
- grad_cross: float32 [256, 256], replicated, may hold values from -6 to 6
- grad_left_two: float32 [256, 4096], P('row', ('col', 'depth')), may hold values from -6 to 6
- grad_left_one: float32 [256, 4096], P('row', ('col', 'depth')), may hold values from -6 to 6
- grad_below: float32 [4096, 4096], P('row', ('col', 'depth')), may hold values from -6 to 6
- grad_panel_two: float32 [4096, 256], P('row', 'col'), may hold values from -6 to 6
- grad_panel_one: float32 [4096, 256], P('row', 'col'), may hold values from -6 to 6
Outputs:
- out_below: float32 [4096, 4096], P('row', ('col', 'depth'))
- out_left_two: float32 [256, 4096], P('row', ('col', 'depth'))
- out_left_one: float32 [256, 4096], P('row', ('col', 'depth'))
- out_diag_two: float32 [256, 256], replicated
- out_diag_one: float32 [256, 256], replicated
- out_cross: float32 [256, 256], replicated
- out_panel_two: float32 [4096, 256], P('row', 'col')
- out_panel_one: float32 [4096, 256], P('row', 'col')
The draws below stay inside these ranges and needn't reach their ends.
Inputs may be any that keep to these rules, and one draw needn't show every extreme that they name: `diag_two`: lower triangular; its diagonal lies in 1 to 3. `diag_one`: lower triangular; its diagonal lies in 1 to 3.
All inputs are finite; a program needn't handle non-finite values.
Results may differ from the reference program's by a relative error of at most 0.000071.
Values sent between devices are 32-bit elements; how exact they have to be, the bound alone decides.
A program may use at most 64 MiB of HBM per device.

```python
import math
import jax
import jax.numpy as jnp
from jax import lax

P_SIZE = 256
M = 4096
J = 4096


def lower_factor(key):
    first, second = jax.random.split(key)
    diagonal = jnp.exp(jax.random.uniform(first, (P_SIZE,), jnp.float32, 0.0, math.log(3.0)))
    below = jnp.clip(jax.random.normal(second, (P_SIZE, P_SIZE), jnp.float32), -5.0, 5.0) * (0.5 / math.sqrt(P_SIZE))
    return jnp.tril(below, -1) + jnp.diag(diagonal)


def draw_diag_two(key, part):
    return lower_factor(jax.random.fold_in(key, 2))


def draw_diag_one(key, part):
    return lower_factor(jax.random.fold_in(key, 1))


def steps_of(key, extent, shards, low, largest):
    loudness = 1.0
    for axis_at, parts in shards:
        heights = jax.random.uniform(jax.random.fold_in(jax.random.fold_in(key, 6), axis_at), (parts,), jnp.float32, low / len(shards), largest / len(shards))
        loudness = loudness * jnp.repeat(jnp.exp(heights), extent[axis_at] // parts).reshape((-1,) + (1,) * (len(extent) - 1 - axis_at))
    return loudness


def scatter_about(stream_key, dims, scale, limit, cuts=(), held_as=jnp.bfloat16):
    level = steps_of(stream_key, dims, cuts, -0.22, 0.18) if cuts else 1.0
    drawn = jax.random.normal(stream_key, dims, jnp.float32) * scale * level
    return jnp.minimum(jnp.maximum(drawn, -limit), limit).astype(held_as)


def setup_inputs(seed: int = 0) -> dict:
    streams_of = jax.random.split(jax.random.key(seed), 17)
    return {
        "diag_two": draw_diag_two(jax.random.fold_in(streams_of[16], 71), 0),
        "diag_one": draw_diag_one(jax.random.fold_in(streams_of[16], 71), 0),
        "cross_tile": scatter_about(streams_of[2], (P_SIZE, P_SIZE), P_SIZE ** -0.5, 0.375, (), jnp.float32),
        "left_two": scatter_about(streams_of[3], (P_SIZE, J), P_SIZE ** -0.5, 0.375, ((1, 8),), jnp.float32),
        "left_one": scatter_about(streams_of[4], (P_SIZE, J), P_SIZE ** -0.5, 0.375, ((1, 8),), jnp.float32),
        "below_left": scatter_about(streams_of[5], (M, J), M ** -0.5, 0.09375, ((0, 4), (1, 8)), jnp.float32),
        "panel_two": scatter_about(streams_of[6], (M, P_SIZE), M ** -0.5, 0.09375, ((0, 4), (1, 2)), jnp.float32),
        "panel_one": scatter_about(streams_of[7], (M, P_SIZE), M ** -0.5, 0.09375, ((0, 4), (1, 2)), jnp.float32),
        "grad_diag_two": scatter_about(streams_of[8], (P_SIZE, P_SIZE), 1.0, 6.0, (), jnp.float32),
        "grad_diag_one": scatter_about(streams_of[9], (P_SIZE, P_SIZE), 1.0, 6.0, (), jnp.float32),
        "grad_cross": scatter_about(streams_of[10], (P_SIZE, P_SIZE), 1.0, 6.0, (), jnp.float32),
        "grad_left_two": scatter_about(streams_of[11], (P_SIZE, J), 1.0, 6.0, ((0, 4), (1, 8)), jnp.float32),
        "grad_left_one": scatter_about(streams_of[12], (P_SIZE, J), 1.0, 6.0, ((0, 4), (1, 8)), jnp.float32),
        "grad_below": scatter_about(streams_of[13], (M, J), 1.0, 6.0, ((0, 4), (1, 8)), jnp.float32),
        "grad_panel_two": scatter_about(streams_of[14], (M, P_SIZE), 1.0, 6.0, ((0, 4), (1, 2)), jnp.float32),
        "grad_panel_one": scatter_about(streams_of[15], (M, P_SIZE), 1.0, 6.0, ((0, 4), (1, 2)), jnp.float32),
    }


def matmul(left, right):
    return jnp.dot(left.astype(jnp.float32), right.astype(jnp.float32), precision=lax.Precision.HIGHEST, preferred_element_type=jnp.float32)

def right_solve(factor, values):
    return lax.linalg.triangular_solve(factor, values, left_side=False, lower=True)

def halved(square):
    return jnp.tril(square) - 0.5 * jnp.diag(jnp.diag(square))

def reverse_block(factor, cotangent):
    inner = halved(matmul(factor.T, cotangent))
    leftward = lax.linalg.triangular_solve(factor, inner, left_side=True, lower=True, transpose_a=True)
    spread = right_solve(factor, leftward)
    return spread + spread.T

def reference(diag_two, diag_one, cross_tile, left_two, left_one, below_left, panel_two, panel_one, grad_diag_two, grad_diag_one, grad_cross, grad_left_two, grad_left_one, grad_below, grad_panel_two, grad_panel_one):
    solved_two = right_solve(diag_two, grad_panel_two)
    below_first = grad_below - matmul(solved_two, left_two)
    panel_next = grad_panel_one - matmul(solved_two, cross_tile)
    gram_two = matmul(solved_two.T, panel_two)
    gram_cross = matmul(solved_two.T, panel_one)
    sym_two = reverse_block(diag_two, grad_diag_two - jnp.tril(gram_two))
    cross_next = grad_cross - gram_cross - matmul(sym_two, cross_tile)
    out_cross = right_solve(diag_one, cross_next)
    out_panel_one = right_solve(diag_one, panel_next)
    out_below = below_first - matmul(out_panel_one, left_one)
    gram_one = matmul(out_cross.T, cross_tile) + matmul(out_panel_one.T, panel_one)
    sym_one = reverse_block(diag_one, grad_diag_one - jnp.tril(gram_one))
    out_left_two = grad_left_two - matmul(solved_two.T, below_left) - matmul(sym_two, left_two) - matmul(out_cross, left_one)
    out_left_one = grad_left_one - matmul(out_cross.T, left_two) - matmul(out_panel_one.T, below_left) - matmul(sym_one, left_one)
    return (out_below, out_left_two, out_left_one, halved(sym_two), halved(sym_one), out_cross, solved_two, out_panel_one)
```

```python
import jax
import jax.numpy as jnp
from jax import lax
from jax.experimental import pallas as pl
from jax.experimental.pallas import tpu as pltpu
from jax.sharding import PartitionSpec as P


def large(left, right, contract):
    return lax.dot_general(
        left,
        right,
        ((contract[:1], contract[1:]), ((), ())),
        precision=lax.Precision.HIGH,
        preferred_element_type=jnp.float32,
    )


def small(left, right, contract=(1, 0)):
    return lax.dot_general(
        left,
        right,
        ((contract[:1], contract[1:]), ((), ())),
        precision=lax.Precision.HIGHEST,
        preferred_element_type=jnp.float32,
    )


def grid_of(size):
    rows = lax.broadcasted_iota(jnp.int32, (size, size), 0)
    cols = lax.broadcasted_iota(jnp.int32, (size, size), 1)
    return rows, cols


def invert_all(blocks):
    size = blocks[0].shape[0]
    rows, cols = grid_of(size)
    apart = rows ^ cols
    lower = rows > cols
    inverses = []
    for block in blocks:
        diagonal = jnp.where(rows == cols, block, 0.0)
        down = 1.0 / jnp.sum(diagonal, axis=1, keepdims=True)
        across = 1.0 / jnp.sum(diagonal, axis=0, keepdims=True)
        pair = jnp.where(lower & (apart == 1), block, 0.0)
        inverses.append(jnp.where(rows == cols, down, 0.0) - pair * down * across)
    level = 1
    while (2 << level) <= size:
        mask = lower & ((apart >> level) == 1)
        steps = [
            small(jnp.where(mask, block, 0.0), inverse) for block, inverse in zip(blocks, inverses)
        ]
        inverses = [inverse - small(inverse, step) for inverse, step in zip(inverses, steps)]
        level += 1
    return inverses


def invert_kernel(two_ref, one_ref, cross_ref, inv_two_ref, inv_one_ref, cross_inv_ref):
    half = two_ref.shape[0] // 2
    refs = (two_ref, one_ref)
    outs = (inv_two_ref, inv_one_ref)
    blocks = []
    for ref in refs:
        blocks += [ref[:half, :half], ref[half:, half:]]
    inverses = invert_all(blocks)
    steps = [small(ref[half:, :half], inverses[2 * at]) for at, ref in enumerate(refs)]
    for at, out in enumerate(outs):
        out[:half, :half] = inverses[2 * at]
        out[half:, half:] = inverses[2 * at + 1]
        out[:half, half:] = jnp.zeros((half, half), jnp.float32)
        out[half:, :half] = -small(inverses[2 * at + 1], steps[at])
    cross_inv_ref[...] = small(cross_ref[...], inv_one_ref[...])


def chain_kernel(
    two_ref,
    one_ref,
    cross_ref,
    inv_two_ref,
    inv_one_ref,
    grad_two_ref,
    grad_one_ref,
    grad_cross_ref,
    place_ref,
    *rest,
):
    grams, outs = rest[:-5], rest[-5:]
    chain(
        two_ref,
        one_ref,
        cross_ref,
        inv_two_ref,
        inv_one_ref,
        grad_two_ref,
        grad_one_ref,
        grad_cross_ref,
        joined(grams, place_ref),
        *outs,
    )


def joined(grams, place_ref):
    if len(grams) == 1:
        return grams[0][...]
    mine, beside, twin, across = [gram[...] for gram in grams]
    left = place_ref[0] == 0
    upper = place_ref[1] == 0
    own = jnp.concatenate([jnp.where(left, mine, beside), jnp.where(left, beside, mine)], axis=1)
    far = jnp.concatenate([jnp.where(left, twin, across), jnp.where(left, across, twin)], axis=1)
    return jnp.concatenate([jnp.where(upper, own, far), jnp.where(upper, far, own)], axis=0)


def chain(
    two_ref,
    one_ref,
    cross_ref,
    inv_two_ref,
    inv_one_ref,
    grad_two_ref,
    grad_one_ref,
    grad_cross_ref,
    grams,
    sym_two_ref,
    sym_one_ref,
    half_two_ref,
    half_one_ref,
    out_cross_ref,
):
    size = two_ref.shape[0]
    rows, cols = grid_of(size)
    lower = rows >= cols
    scale = jnp.where(rows > cols, 1.0, jnp.where(rows == cols, 0.5, 0.0))

    def sym(factor, inverse, cotangent):
        inner = scale * small(factor, cotangent, (0, 0))
        spread = small(small(inverse, inner, (0, 0)), inverse)
        return spread + spread.T

    gram_two = grams[:size, :]
    gram_cross = grams[size : 2 * size, :]
    gram_below = grams[2 * size :, :]
    sym_two = sym(
        two_ref[...], inv_two_ref[...], grad_two_ref[...] - jnp.where(lower, gram_two, 0.0)
    )
    sym_two_ref[...] = sym_two
    half_two_ref[...] = scale * sym_two
    cross_next = grad_cross_ref[...] - gram_cross - small(sym_two, cross_ref[...])
    out_cross = small(cross_next, inv_one_ref[...])
    out_cross_ref[...] = out_cross
    gram_one = small(out_cross, cross_ref[...], (0, 0)) + gram_below
    sym_one = sym(
        one_ref[...], inv_one_ref[...], grad_one_ref[...] - jnp.where(lower, gram_one, 0.0)
    )
    sym_one_ref[...] = sym_one
    half_one_ref[...] = scale * sym_one


def local_call(kernel, operands, count, flops):
    size = operands[0].shape[0]
    moved = 4 * size * size * (len(operands) + count)
    return pl.pallas_call(
        kernel,
        out_shape=[jax.ShapeDtypeStruct((size, size), jnp.float32)] * count,
        in_specs=[
            pl.BlockSpec(memory_space=pltpu.SMEM if operand.ndim == 1 else pltpu.VMEM)
            for operand in operands
        ],
        out_specs=[pl.BlockSpec(memory_space=pltpu.VMEM)] * count,
        cost_estimate=pl.CostEstimate(flops=flops, bytes_accessed=moved, transcendentals=0),
    )(*operands)


def swap(values, axis, bit):
    size = lax.axis_size(axis)
    return lax.ppermute(values, axis, [(at, at ^ bit) for at in range(size)])


def gathered(values, axis):
    if lax.axis_size(axis) != 2:
        return [(lax.all_gather(values, axis, axis=1, tiled=True), 0)]
    width = values.shape[1]
    at = lax.axis_index(axis)
    return [(values, at * width), (swap(values, axis, 1), (1 - at) * width)]


def parted(values):
    high = values.astype(jnp.bfloat16)
    return high, (values - high.astype(jnp.float32)).astype(jnp.bfloat16)


def product(left, right):
    (left_high, left_low), (right_high, right_low) = parted(left), parted(right)

    def single(one, other):
        return jnp.dot(one, other, preferred_element_type=jnp.float32)

    return (single(left_low, right_high) + single(left_high, right_low)) + single(
        left_high, right_high
    )


def solve_kernel(count, starts_ref, inverse_ref, *refs):
    pieces, extra, outs = refs[:count], refs[count:-count], refs[-count:]
    total = None
    for at, piece in enumerate(pieces):
        width = piece.shape[1]
        rows = inverse_ref[pl.ds(pl.multiple_of(starts_ref[at], width), width), :]
        part = product(piece[...], rows)
        total = part if total is None else total + part
    if extra:
        total = total - product(extra[0][...], extra[1][...])
    outs[0][...] = total
    if count > 1:
        width = outs[1].shape[1]
        outs[1][...] = jnp.where(starts_ref[0] == 0, total[:, :width], total[:, width:])


def solve(pieces, inverse, *extra):
    count = len(pieces)
    rows, width = pieces[0][0].shape
    size = inverse.shape[0]
    block = rows // 4
    starts = jnp.stack([jnp.asarray(start, jnp.int32) for _, start in pieces])

    def tall(columns):
        return pl.BlockSpec((block, columns), lambda step: (step, 0))

    whole = pl.BlockSpec((size, size), lambda step: (0, 0))
    widths = [size, width][:count]
    return pl.pallas_call(
        lambda *refs: solve_kernel(count, *refs),
        grid=(4,),
        out_shape=[jax.ShapeDtypeStruct((rows, columns), jnp.float32) for columns in widths],
        in_specs=[pl.BlockSpec(memory_space=pltpu.SMEM), whole]
        + [tall(values.shape[1]) for values, _ in pieces]
        + ([tall(size), whole] if extra else []),
        out_specs=[tall(columns) for columns in widths],
        cost_estimate=pl.CostEstimate(
            flops=6 * rows * size * size, bytes_accessed=12 * rows * size, transcendentals=0
        ),
    )(starts, inverse, *[values for values, _ in pieces], *extra)


def assembled(values, axis):
    size = lax.axis_size(axis)
    if size != 2:
        return lax.all_gather(values, axis, axis=1, tiled=True)
    other = swap(values, axis, 1)
    first = lax.axis_index(axis) == 0
    return jnp.concatenate(
        [jnp.where(first, values, other), jnp.where(first, other, values)], axis=1
    )


def halve(values, axis, bit):
    mine = (lax.axis_index(axis) // bit) % 2
    keep = lax.dynamic_index_in_dim(values, mine, 0, keepdims=False)
    give = lax.dynamic_index_in_dim(values, 1 - mine, 0, keepdims=False)
    return keep + swap(give, axis, bit)


def scatter_sum(values, axis):
    size = lax.axis_size(axis)
    if size & (size - 1):
        return lax.psum_scatter(values, axis, scatter_dimension=0, tiled=False)
    bit = 1
    while bit < size:
        paired = values.reshape((-1, 2) + values.shape[1:])
        values = halve(jnp.moveaxis(paired, 1, 0), axis, bit)
        bit *= 2
    return values[0]


def row_sum(values, axis, columns):
    size = lax.axis_size(axis)
    if size & (size - 1) or size < 2:
        return [assembled(lax.psum(values, axis), columns)]
    part = halve(values.reshape((2, -1) + values.shape[1:]), axis, 1)
    bit = 2
    while bit < size:
        part = part + swap(part, axis, bit)
        bit *= 2
    if lax.axis_size(columns) == 2:
        beside = swap(part, columns, 1)
        return [part, beside, swap(part, axis, 1), swap(beside, axis, 1)]
    part = assembled(part, columns)
    other = swap(part, axis, 1)
    even = lax.axis_index(axis) % 2 == 0
    return [jnp.concatenate([jnp.where(even, part, other), jnp.where(even, other, part)], axis=0)]


def body(
    diag_two,
    diag_one,
    cross_tile,
    left_two,
    left_one,
    below_left,
    panel_two,
    panel_one,
    grad_diag_two,
    grad_diag_one,
    grad_cross,
    grad_left_two,
    grad_left_one,
    grad_below,
    grad_panel_two,
    grad_panel_one,
):
    size = diag_two.shape[0]
    share = grad_left_two.shape[0]
    width = panel_two.shape[1]
    row_start = lax.axis_index("row") * share
    col_start = lax.axis_index("col") * width
    cube = 2 * size**3

    pieces_two = gathered(grad_panel_two, "col")
    pieces_one = gathered(grad_panel_one, "col")
    inv_two, inv_one, cross_inv = local_call(
        invert_kernel, (diag_two, diag_one, cross_tile), 3, 60 * cube
    )
    solved_two, *own_two = solve(pieces_two, inv_two)
    solved_one, *own_one = solve(pieces_one, inv_one, solved_two, cross_inv)
    place = jnp.stack([lax.axis_index("col"), lax.axis_index("row") % 2]).astype(jnp.int32)
    partial = jnp.concatenate(
        [
            large(solved_two, panel_two, (0, 0)),
            large(solved_two, panel_one, (0, 0)),
            large(solved_one, panel_one, (0, 0)),
        ],
        axis=0,
    )
    grams = row_sum(partial, "row", "col")
    rows = lax.axis_size("row")
    lefts = jnp.stack(
        [
            large(solved_two, below_left, (0, 0)).reshape(rows, share, -1),
            large(solved_one, below_left, (0, 0)).reshape(rows, share, -1),
        ],
        axis=1,
    )
    summed = scatter_sum(lefts, "row")
    out_below = (
        grad_below - large(solved_two, left_two, (1, 0)) - large(solved_one, left_one, (1, 0))
    )
    sym_two, sym_one, half_two, half_one, out_cross = local_call(
        chain_kernel,
        (
            diag_two,
            diag_one,
            cross_tile,
            inv_two,
            inv_one,
            grad_diag_two,
            grad_diag_one,
            grad_cross,
            place,
            *grams,
        ),
        5,
        60 * cube,
    )
    sym_two_rows = lax.dynamic_slice_in_dim(sym_two, row_start, share, 0)
    sym_one_rows = lax.dynamic_slice_in_dim(sym_one, row_start, share, 0)
    cross_rows = lax.dynamic_slice_in_dim(out_cross, row_start, share, 0)
    cross_cols = lax.dynamic_slice_in_dim(out_cross, row_start, share, 1)
    out_left_two = (
        grad_left_two
        - summed[0]
        - large(sym_two_rows, left_two, (1, 0))
        - large(cross_rows, left_one, (1, 0))
    )
    out_left_one = (
        grad_left_one
        - summed[1]
        - large(cross_cols, left_two, (0, 0))
        - large(sym_one_rows, left_one, (1, 0))
    )
    return (
        out_below,
        out_left_two,
        out_left_one,
        half_two,
        half_one,
        out_cross,
        own_two[0] if own_two else lax.dynamic_slice_in_dim(solved_two, col_start, width, 1),
        own_one[0] if own_one else lax.dynamic_slice_in_dim(solved_one, col_start, width, 1),
    )


MESH = pl.DeviceIdType.MESH


def split(values):
    high = values.astype(jnp.bfloat16)
    return high, (values - high.astype(jnp.float32)).astype(jnp.bfloat16)


def thrice(left, right, contract=(1, 0)):
    def single(one, other):
        return lax.dot_general(
            one,
            other,
            ((contract[:1], contract[1:]), ((), ())),
            preferred_element_type=jnp.float32,
        )

    return (single(left[1], right[0]) + single(left[0], right[1])) + single(left[0], right[0])


def fused_kernel(chunks, *refs):
    (
        two_hbm,
        one_hbm,
        cross_hbm,
        left_two_hbm,
        left_one_hbm,
        below_hbm,
        panel_two_hbm,
        panel_one_hbm,
        grad_two_hbm,
        grad_one_hbm,
        grad_cross_hbm,
        grad_left_two_hbm,
        grad_left_one_hbm,
        grad_below_hbm,
        grad_panel_two_hbm,
        grad_panel_one_hbm,
    ) = refs[:16]
    (
        out_below,
        out_left_two,
        out_left_one,
        out_diag_two,
        out_diag_one,
        out_cross,
        out_panel_two,
        out_panel_one,
    ) = refs[16:24]
    (
        two,
        one,
        cross,
        left,
        below,
        panels,
        grad_two,
        grad_one,
        grad_cross,
        grad_left,
        acc,
        full_two,
        full_one,
        solved,
        solved_high,
        solved_low,
        left_high,
        left_low,
        below_high,
        below_low,
        inverses,
        crossed,
        pre,
        partial,
        from_core,
        chip,
        from_x,
        own,
        oth,
        lefts,
        lefts_core,
        lefts_send,
        lefts_x,
        sym,
        next_cross,
        cross_t,
        halves,
        panel_out,
        load_sem,
        store_sem,
        y_send,
        y_recv,
        z_send,
        z_recv,
        w_send,
        w_recv,
        l_send,
        l_recv,
    ) = refs[24:]
    size = two.shape[0]
    rows, width = grad_panel_two_hbm.shape
    share = grad_left.shape[1]
    half = rows // 2
    step = half // chunks
    quarter = width // 2
    at_row, at_col, at_depth = (lax.axis_index(name) for name in ("row", "col", "depth"))
    core = lax.rem(at_row, 2)
    side = lax.div(at_row, 2)
    first = at_col == 0
    part = lax.rem(at_depth, 2)
    to_core = (at_row + 1 - 2 * core, at_col, at_depth)
    to_x = (at_row + 2 - 4 * side, at_col, at_depth)
    to_y = (at_row, 1 - at_col, at_depth)
    to_z = (at_row, at_col, at_depth + 1 - 2 * part)

    loads = []

    def load(source, target):
        copy = pltpu.make_async_copy(source, target, load_sem.at[len(loads)])
        copy.start()
        loads.append(copy)
        return copy

    own_two = load(grad_panel_two_hbm, full_two.at[:, :width])
    pan_two = load(panel_two_hbm, panels.at[:, :width])
    pan_one = load(panel_one_hbm, panels.at[:, width:])
    own_one = load(grad_panel_one_hbm, full_one.at[:, :width])
    small_loads = [
        load(two_hbm, two),
        load(one_hbm, one),
        load(cross_hbm, cross),
        load(grad_two_hbm, grad_two),
        load(grad_one_hbm, grad_one),
        load(grad_cross_hbm, grad_cross),
    ]
    below_load = load(below_hbm, below)
    left_loads = [load(left_two_hbm, left.at[:size]), load(left_one_hbm, left.at[size:])]
    acc_load = load(grad_below_hbm, acc)
    grad_left_loads = [
        load(grad_left_two_hbm, grad_left.at[0]),
        load(grad_left_one_hbm, grad_left.at[1]),
    ]

    barrier = pltpu.get_barrier_semaphore()
    for target in (to_core, to_x, to_y, to_z):
        pl.semaphore_signal(barrier, inc=1, device_id=target, device_id_type=MESH)
    pl.semaphore_wait(barrier, 4)

    sends = []

    def send(source, target, sems, at, device):
        copy = pltpu.make_async_remote_copy(
            src_ref=source,
            dst_ref=target,
            send_sem=sems[0].at[at],
            recv_sem=sems[1].at[at],
            device_id=device,
            device_id_type=MESH,
        )
        copy.start()
        sends.append(copy)
        return copy

    fulls = (full_two, full_one)
    y_copies = []
    for panel, source in enumerate((grad_panel_two_hbm, grad_panel_one_hbm)):
        for at in range(chunks):
            place = pl.ds(pl.multiple_of(part * half + at * step, step), step)
            y_copies.append(
                send(
                    source.at[place, :],
                    fulls[panel].at[place, width:],
                    (y_send, y_recv),
                    panel * chunks + at,
                    to_y,
                )
            )
    z_copies = []

    def forward():
        at = len(z_copies)
        y_copies[at].wait_recv()
        panel, chunk = divmod(at, chunks)
        place = pl.ds(pl.multiple_of(part * half + chunk * step, step), step)
        piece = fulls[panel].at[place, width:]
        z_copies.append(send(piece, piece, (z_send, z_recv), at, to_z))

    mine = pl.ds(pl.multiple_of(core * quarter, quarter), quarter)
    theirs = pl.ds(pl.multiple_of((1 - core) * quarter, quarter), quarter)
    stages = ((0, 3), (3, 2), (5, 1))
    waits = {}

    def w_core(stage):
        start, count = stages[stage]
        blocks = pl.ds(start, count)
        waits["core", stage] = send(
            partial.at[blocks, theirs, :],
            from_core.at[blocks],
            (w_send, w_recv),
            stage * 5,
            to_core,
        )

    def w_x(stage):
        start, count = stages[stage]
        blocks = pl.ds(start, count)
        waits["core", stage].wait_recv()
        chip[blocks] = partial[blocks, mine, :] + from_core[blocks]
        waits["x", stage] = send(
            chip.at[blocks], from_x.at[blocks], (w_send, w_recv), stage * 5 + 1, to_x
        )

    def w_y(stage):
        start, count = stages[stage]
        blocks = pl.ds(start, count)
        waits["x", stage].wait_recv()
        own[blocks, mine, :] = chip[blocks] + from_x[blocks]
        piece = own.at[blocks, mine, :]
        waits["y", stage] = send(
            piece, oth.at[blocks, mine, :], (w_send, w_recv), stage * 5 + 2, to_y
        )
        waits["own", stage] = send(piece, piece, (w_send, w_recv), stage * 5 + 3, to_core)

    def w_last(stage):
        start, count = stages[stage]
        blocks = pl.ds(start, count)
        waits["y", stage].wait_recv()
        piece = oth.at[blocks, mine, :]
        waits["oth", stage] = send(piece, piece, (w_send, w_recv), stage * 5 + 4, to_core)

    def w_done(stage):
        waits["own", stage].wait_recv()
        waits["oth", stage].wait_recv()

    def joined_at(diagonal, off):
        near, far = own[diagonal], oth[diagonal]
        near_off, far_off = own[off], oth[off]
        top = [jnp.where(first, near, far), jnp.where(first, far_off, near_off)]
        bottom = [jnp.where(first, near_off, far_off), jnp.where(first, far, near)]
        return jnp.concatenate(
            [jnp.concatenate(top, axis=1), jnp.concatenate(bottom, axis=1)], axis=0
        )

    own_two.wait()
    pan_two.wait()
    pan_one.wait()
    panel_parts = split(panels[...])
    found = thrice(split(full_two[:, :width]), panel_parts, (0, 0))
    partial[0] = found[:, :width]
    partial[1] = found[:, width:]
    own_one.wait()
    partial[2] = thrice(
        split(full_one[:, :width]), tuple(piece[:, width:] for piece in panel_parts), (0, 0)
    )
    w_core(0)

    for copy in small_loads:
        copy.wait()
    grid_rows, grid_cols = grid_of(size)
    scale = jnp.where(
        grid_rows > grid_cols, 1.0, jnp.where(grid_rows == grid_cols, 0.5, 0.0)
    )
    events = {1: forward, 2: lambda: w_x(0), 3: forward, 5: forward, 6: lambda: w_y(0)}
    mid = size // 2
    blocks = []
    for ref in (two, one):
        blocks += [ref[:mid, :mid], ref[mid:, mid:]]
    found = invert_steps(blocks, events)
    for at, ref in enumerate((two, one)):
        step_product = small(ref[mid:, :mid], found[2 * at])
        inverses[at, :mid, :mid] = found[2 * at]
        inverses[at, mid:, mid:] = found[2 * at + 1]
        inverses[at, :mid, mid:] = jnp.zeros((mid, size - mid), jnp.float32)
        inverses[at, mid:, :mid] = -small(found[2 * at + 1], step_product)
    while len(z_copies) < chunks:
        forward()

    def local_rows(values):
        near = jnp.where(first, values[:width, :], values[width:, :])
        away = jnp.where(first, values[width:, :], values[:width, :])
        return jnp.concatenate([near, away], axis=0)

    inverse_two = inverses[0]
    right_two = split(local_rows(inverse_two))

    def solve_two(begin):
        place = pl.ds(pl.multiple_of(begin, half), half)
        pieces = split(full_two[place, :])
        off = thrice(
            tuple(piece[:, width:] for piece in pieces), split(panels[place, :]), (0, 0)
        )
        total = thrice(pieces, right_two)
        solved[place, :size] = total
        high, low = split(total)
        solved_high[place, :size] = high
        solved_low[place, :size] = low
        return off

    off_near = solve_two(part * half)
    forward()
    crossed[0] = small(cross[...], inverses[1])
    crossed[1] = small(inverse_two, cross[...])
    pre[0] = small(two[...], grad_two[...], (0, 0))
    pre[1] = small(one[...], grad_one[...], (0, 0))
    for at in range(chunks):
        z_copies[at].wait_recv()
    off_far = solve_two((1 - part) * half)
    off = off_near + off_far
    partial[3] = off[:, :width]
    partial[4] = off[:, width:]
    w_core(1)
    forward()

    stores = []

    def store(source, target):
        copy = pltpu.make_async_copy(source, target, store_sem.at[len(stores)])
        copy.start()
        stores.append(copy)

    def own_columns(values):
        return jnp.where(first, values[:, :width], values[:, width:])

    panel_out[0] = own_columns(solved[:, :size])
    store(panel_out.at[0], out_panel_two)
    below_load.wait()
    high, low = split(below[...])
    below_high[...] = high
    below_low[...] = low
    for copy in left_loads:
        copy.wait()
    high, low = split(left[...])
    left_high[...] = high
    left_low[...] = low
    w_x(1)
    l_waits = {}

    def lefts_of(panel):
        columns = pl.ds(panel * size, size)
        product_of = thrice(
            (solved_high[:, columns], solved_low[:, columns]),
            (below_high[...], below_low[...]),
            (0, 0),
        )
        lefts[panel] = product_of.reshape(lefts.shape[1:])
        for at in range(2):
            l_waits["core", panel, at] = send(
                lefts.at[panel, at, 1 - core],
                lefts_core.at[panel, at],
                (l_send, l_recv),
                panel * 3 + at,
                to_core,
            )

    def lefts_away(panel):
        for at in range(2):
            l_waits["core", panel, at].wait_recv()
        lefts_send[panel] = lefts[panel, 1 - side, core] + lefts_core[panel, 1 - side]
        l_waits["x", panel] = send(
            lefts_send.at[panel], lefts_x.at[panel], (l_send, l_recv), panel * 3 + 2, to_x
        )

    def lefts_end(panel):
        l_waits["x", panel].wait_recv()
        return (lefts[panel, side, core] + lefts_core[panel, side]) + lefts_x[panel]

    tile = rows // 4

    def below_of(panel):
        columns = pl.ds(panel * size, size)
        rights = (left_high[columns, :], left_low[columns, :])
        for at in range(4):
            place = pl.ds(at * tile, tile)
            acc[place, :] = acc[place, :] - thrice(
                (solved_high[place, columns], solved_low[place, columns]), rights
            )

    lefts_of(0)
    forward()
    acc_load.wait()
    below_of(0)
    lefts_away(0)
    forward()
    w_y(1)

    right_one = split(
        jnp.concatenate([local_rows(inverses[1]), -crossed[0]], axis=0)
    )

    def solve_one(begin):
        place = pl.ds(pl.multiple_of(begin, half), half)
        pieces = split(full_one[place, :])
        off = thrice(
            tuple(piece[:, width:] for piece in pieces), split(panels[place, width:]), (0, 0)
        )
        lefts_of_it = tuple(
            jnp.concatenate([piece, before[place, :size]], axis=1)
            for piece, before in zip(pieces, (solved_high, solved_low))
        )
        total = thrice(lefts_of_it, right_one)
        solved[place, size:] = total
        high, low = split(total)
        solved_high[place, size:] = high
        solved_low[place, size:] = low
        return off

    off_near = solve_one(part * half)
    w_last(0)
    for at in range(chunks, 2 * chunks):
        z_copies[at].wait_recv()
    off_far = solve_one((1 - part) * half)
    partial[5] = off_near + off_far
    w_core(2)
    panel_out[1] = own_columns(solved[:, size:])
    store(panel_out.at[1], out_panel_one)
    w_last(1)
    w_x(2)
    lefts_of(1)
    w_y(2)
    w_done(0)
    w_done(1)

    inner = scale * (pre[0] - joined_at(0, 3))
    middle = inner + inner.T
    cross_gram = small(inverse_two, joined_at(1, 4), (0, 0))
    spread = small(
        inverse_two,
        small(middle, jnp.concatenate([inverse_two, crossed[1]], axis=1)),
        (0, 0),
    )
    sym[0] = spread[:, :size]
    halves[0] = scale * sym[0]
    store(halves.at[0], out_diag_two)
    following = grad_cross[...] - cross_gram - spread[:, size:]
    next_cross[...] = small(following, inverses[1])
    store(next_cross, out_cross)
    cross_t[...] = next_cross[...].T
    lefts_away(1)
    ready = pre[1] - (
        small(following, cross[...], (0, 0)) - small(cross[...], cross_gram, (0, 0))
    )
    w_last(2)
    below_of(1)
    store(acc, out_below)
    mine_rows = pl.ds(pl.multiple_of(at_row * share, share), share)
    for copy in grad_left_loads:
        copy.wait()
    head = split(jnp.concatenate([sym[0, mine_rows, :], next_cross[mine_rows, :]], axis=1))
    grad_left[0] = (grad_left[0] - lefts_end(0)) - thrice(
        head, (left_high[...], left_low[...])
    )
    store(grad_left.at[0], out_left_two)
    grad_left[1] = (grad_left[1] - lefts_end(1)) - thrice(
        split(cross_t[mine_rows, :]), (left_high[:size], left_low[:size])
    )
    w_done(2)
    inner = scale * (ready - joined_at(2, 5))
    sym[1] = small(inverses[1], small(inner + inner.T, inverses[1]), (0, 0))
    grad_left[1] = grad_left[1] - thrice(
        split(sym[1, mine_rows, :]), (left_high[size:], left_low[size:])
    )
    store(grad_left.at[1], out_left_one)
    halves[1] = scale * sym[1]
    store(halves.at[1], out_diag_one)
    for copy in sends:
        copy.wait_send()
    for copy in stores:
        copy.wait()


def invert_steps(blocks, events):
    size = blocks[0].shape[0]
    rows, cols = grid_of(size)
    apart = rows ^ cols
    lower = rows > cols
    inverses = []
    for block in blocks:
        diagonal = jnp.where(rows == cols, block, 0.0)
        down = 1.0 / jnp.sum(diagonal, axis=1, keepdims=True)
        across = 1.0 / jnp.sum(diagonal, axis=0, keepdims=True)
        pair = jnp.where(lower & (apart == 1), block, 0.0)
        inverses.append(jnp.where(rows == cols, down, 0.0) - pair * down * across)
    level = 1
    while (2 << level) <= size:
        mask = lower & ((apart >> level) == 1)
        steps = [
            small(jnp.where(mask, block, 0.0), inverse) for block, inverse in zip(blocks, inverses)
        ]
        inverses = [inverse - small(inverse, step) for inverse, step in zip(inverses, steps)]
        if level in events:
            events[level]()
        level += 1
    for late in sorted(events):
        if late >= level:
            events[late]()
    return inverses


def fused(*arrays):
    two, left, below, grad_left = arrays[0], arrays[3], arrays[5], arrays[11]
    size = two.shape[0]
    rows, width = arrays[14].shape
    columns = below.shape[1]
    share = grad_left.shape[0]
    chunks = 4
    quarter = width // 2

    def real(*shape):
        return pltpu.VMEM(shape, jnp.float32)

    def short(*shape):
        return pltpu.VMEM(shape, jnp.bfloat16)

    def outs(*shape):
        return jax.ShapeDtypeStruct(shape, jnp.float32)

    scratch = [
        real(size, size),
        real(size, size),
        real(size, size),
        real(2 * size, columns),
        real(rows, columns),
        real(rows, size),
        real(size, size),
        real(size, size),
        real(size, size),
        real(2, share, columns),
        real(rows, columns),
        real(rows, size),
        real(rows, size),
        real(rows, 2 * size),
        short(rows, 2 * size),
        short(rows, 2 * size),
        short(2 * size, columns),
        short(2 * size, columns),
        short(rows, columns),
        short(rows, columns),
        real(2, size, size),
        real(2, size, size),
        real(2, size, size),
        real(6, width, width),
        real(6, quarter, width),
        real(6, quarter, width),
        real(6, quarter, width),
        real(6, width, width),
        real(6, width, width),
        real(2, 2, 2, share, columns),
        real(2, 2, share, columns),
        real(2, share, columns),
        real(2, share, columns),
        real(2, size, size),
        real(size, size),
        real(size, size),
        real(2, size, size),
        real(2, rows, width),
        pltpu.SemaphoreType.DMA((16,)),
        pltpu.SemaphoreType.DMA((8,)),
        pltpu.SemaphoreType.DMA((2 * chunks,)),
        pltpu.SemaphoreType.DMA((2 * chunks,)),
        pltpu.SemaphoreType.DMA((2 * chunks,)),
        pltpu.SemaphoreType.DMA((2 * chunks,)),
        pltpu.SemaphoreType.DMA((15,)),
        pltpu.SemaphoreType.DMA((15,)),
        pltpu.SemaphoreType.DMA((6,)),
        pltpu.SemaphoreType.DMA((6,)),
    ]
    anywhere = pl.BlockSpec(memory_space=pl.ANY)
    return pl.pallas_call(
        lambda *refs: fused_kernel(chunks, *refs),
        out_shape=[
            outs(rows, columns),
            outs(share, columns),
            outs(share, columns),
            outs(size, size),
            outs(size, size),
            outs(size, size),
            outs(rows, width),
            outs(rows, width),
        ],
        in_specs=[anywhere] * 16,
        out_specs=[anywhere] * 8,
        scratch_shapes=scratch,
        compiler_params=pltpu.CompilerParams(collective_id=0, has_side_effects=True),
        cost_estimate=pl.CostEstimate(
            flops=24 * rows * size * columns, bytes_accessed=16 * rows * columns, transcendentals=0
        ),
    )(*arrays)


def fits(mesh):
    return mesh.shape["row"] == 4 and mesh.shape["col"] == 2 and mesh.shape["depth"] % 2 == 0


def solution(mesh):
    panels = P("row", "col")
    lefts = P(None, ("col", "depth"))
    blocks = P("row", ("col", "depth"))
    return jax.shard_map(
        fused if fits(mesh) else body,
        mesh=mesh,
        in_specs=(P(), P(), P(), lefts, lefts, blocks, panels, panels)
        + (P(), P(), P(), blocks, blocks, blocks, panels, panels),
        out_specs=(blocks, blocks, blocks, P(), P(), P(), panels, panels),
        check_vma=False,
    )
```

```python
import jax
import jax.numpy as jnp
from jax import lax
from jax.experimental import pallas as pl
from jax.experimental.pallas import tpu as pltpu
from jax.sharding import PartitionSpec as P


def large(left, right, contract):
    return lax.dot_general(
        left,
        right,
        ((contract[:1], contract[1:]), ((), ())),
        precision=lax.Precision.HIGH,
        preferred_element_type=jnp.float32,
    )


def small(left, right, contract=(1, 0)):
    return lax.dot_general(
        left,
        right,
        ((contract[:1], contract[1:]), ((), ())),
        precision=lax.Precision.HIGHEST,
        preferred_element_type=jnp.float32,
    )


def grid_of(size):
    rows = lax.broadcasted_iota(jnp.int32, (size, size), 0)
    cols = lax.broadcasted_iota(jnp.int32, (size, size), 1)
    return rows, cols


def invert_all(blocks):
    size = blocks[0].shape[0]
    rows, cols = grid_of(size)
    apart = rows ^ cols
    lower = rows > cols
    inverses = []
    for block in blocks:
        diagonal = jnp.where(rows == cols, block, 0.0)
        down = 1.0 / jnp.sum(diagonal, axis=1, keepdims=True)
        across = 1.0 / jnp.sum(diagonal, axis=0, keepdims=True)
        pair = jnp.where(lower & (apart == 1), block, 0.0)
        inverses.append(jnp.where(rows == cols, down, 0.0) - pair * down * across)
    level = 1
    while (2 << level) <= size:
        mask = lower & ((apart >> level) == 1)
        steps = [
            small(jnp.where(mask, block, 0.0), inverse) for block, inverse in zip(blocks, inverses)
        ]
        inverses = [inverse - small(inverse, step) for inverse, step in zip(inverses, steps)]
        level += 1
    return inverses


def invert_kernel(two_ref, one_ref, cross_ref, inv_two_ref, inv_one_ref, cross_inv_ref):
    half = two_ref.shape[0] // 2
    refs = (two_ref, one_ref)
    outs = (inv_two_ref, inv_one_ref)
    blocks = []
    for ref in refs:
        blocks += [ref[:half, :half], ref[half:, half:]]
    inverses = invert_all(blocks)
    steps = [small(ref[half:, :half], inverses[2 * at]) for at, ref in enumerate(refs)]
    for at, out in enumerate(outs):
        out[:half, :half] = inverses[2 * at]
        out[half:, half:] = inverses[2 * at + 1]
        out[:half, half:] = jnp.zeros((half, half), jnp.float32)
        out[half:, :half] = -small(inverses[2 * at + 1], steps[at])
    cross_inv_ref[...] = small(cross_ref[...], inv_one_ref[...])


def chain_kernel(
    two_ref,
    one_ref,
    cross_ref,
    inv_two_ref,
    inv_one_ref,
    grad_two_ref,
    grad_one_ref,
    grad_cross_ref,
    place_ref,
    *rest,
):
    grams, outs = rest[:-5], rest[-5:]
    chain(
        two_ref,
        one_ref,
        cross_ref,
        inv_two_ref,
        inv_one_ref,
        grad_two_ref,
        grad_one_ref,
        grad_cross_ref,
        joined(grams, place_ref),
        *outs,
    )


def joined(grams, place_ref):
    if len(grams) == 1:
        return grams[0][...]
    mine, beside, twin, across = [gram[...] for gram in grams]
    left = place_ref[0] == 0
    upper = place_ref[1] == 0
    own = jnp.concatenate([jnp.where(left, mine, beside), jnp.where(left, beside, mine)], axis=1)
    far = jnp.concatenate([jnp.where(left, twin, across), jnp.where(left, across, twin)], axis=1)
    return jnp.concatenate([jnp.where(upper, own, far), jnp.where(upper, far, own)], axis=0)


def chain(
    two_ref,
    one_ref,
    cross_ref,
    inv_two_ref,
    inv_one_ref,
    grad_two_ref,
    grad_one_ref,
    grad_cross_ref,
    grams,
    sym_two_ref,
    sym_one_ref,
    half_two_ref,
    half_one_ref,
    out_cross_ref,
):
    size = two_ref.shape[0]
    rows, cols = grid_of(size)
    lower = rows >= cols
    scale = jnp.where(rows > cols, 1.0, jnp.where(rows == cols, 0.5, 0.0))

    def sym(factor, inverse, cotangent):
        inner = scale * small(factor, cotangent, (0, 0))
        spread = small(small(inverse, inner, (0, 0)), inverse)
        return spread + spread.T

    gram_two = grams[:size, :]
    gram_cross = grams[size : 2 * size, :]
    gram_below = grams[2 * size :, :]
    sym_two = sym(
        two_ref[...], inv_two_ref[...], grad_two_ref[...] - jnp.where(lower, gram_two, 0.0)
    )
    sym_two_ref[...] = sym_two
    half_two_ref[...] = scale * sym_two
    cross_next = grad_cross_ref[...] - gram_cross - small(sym_two, cross_ref[...])
    out_cross = small(cross_next, inv_one_ref[...])
    out_cross_ref[...] = out_cross
    gram_one = small(out_cross, cross_ref[...], (0, 0)) + gram_below
    sym_one = sym(
        one_ref[...], inv_one_ref[...], grad_one_ref[...] - jnp.where(lower, gram_one, 0.0)
    )
    sym_one_ref[...] = sym_one
    half_one_ref[...] = scale * sym_one


def local_call(kernel, operands, count, flops):
    size = operands[0].shape[0]
    moved = 4 * size * size * (len(operands) + count)
    return pl.pallas_call(
        kernel,
        out_shape=[jax.ShapeDtypeStruct((size, size), jnp.float32)] * count,
        in_specs=[
            pl.BlockSpec(memory_space=pltpu.SMEM if operand.ndim == 1 else pltpu.VMEM)
            for operand in operands
        ],
        out_specs=[pl.BlockSpec(memory_space=pltpu.VMEM)] * count,
        cost_estimate=pl.CostEstimate(flops=flops, bytes_accessed=moved, transcendentals=0),
    )(*operands)


def swap(values, axis, bit):
    size = lax.axis_size(axis)
    return lax.ppermute(values, axis, [(at, at ^ bit) for at in range(size)])


def gathered(values, axis):
    if lax.axis_size(axis) != 2:
        return [(lax.all_gather(values, axis, axis=1, tiled=True), 0)]
    width = values.shape[1]
    at = lax.axis_index(axis)
    return [(values, at * width), (swap(values, axis, 1), (1 - at) * width)]


def parted(values):
    high = values.astype(jnp.bfloat16)
    return high, (values - high.astype(jnp.float32)).astype(jnp.bfloat16)


def product(left, right):
    (left_high, left_low), (right_high, right_low) = parted(left), parted(right)

    def single(one, other):
        return jnp.dot(one, other, preferred_element_type=jnp.float32)

    return (single(left_low, right_high) + single(left_high, right_low)) + single(
        left_high, right_high
    )


def solve_kernel(count, starts_ref, inverse_ref, *refs):
    pieces, extra, outs = refs[:count], refs[count:-count], refs[-count:]
    total = None
    for at, piece in enumerate(pieces):
        width = piece.shape[1]
        rows = inverse_ref[pl.ds(pl.multiple_of(starts_ref[at], width), width), :]
        part = product(piece[...], rows)
        total = part if total is None else total + part
    if extra:
        total = total - product(extra[0][...], extra[1][...])
    outs[0][...] = total
    if count > 1:
        width = outs[1].shape[1]
        outs[1][...] = jnp.where(starts_ref[0] == 0, total[:, :width], total[:, width:])


def solve(pieces, inverse, *extra):
    count = len(pieces)
    rows, width = pieces[0][0].shape
    size = inverse.shape[0]
    block = rows // 4
    starts = jnp.stack([jnp.asarray(start, jnp.int32) for _, start in pieces])

    def tall(columns):
        return pl.BlockSpec((block, columns), lambda step: (step, 0))

    whole = pl.BlockSpec((size, size), lambda step: (0, 0))
    widths = [size, width][:count]
    return pl.pallas_call(
        lambda *refs: solve_kernel(count, *refs),
        grid=(4,),
        out_shape=[jax.ShapeDtypeStruct((rows, columns), jnp.float32) for columns in widths],
        in_specs=[pl.BlockSpec(memory_space=pltpu.SMEM), whole]
        + [tall(values.shape[1]) for values, _ in pieces]
        + ([tall(size), whole] if extra else []),
        out_specs=[tall(columns) for columns in widths],
        cost_estimate=pl.CostEstimate(
            flops=6 * rows * size * size, bytes_accessed=12 * rows * size, transcendentals=0
        ),
    )(starts, inverse, *[values for values, _ in pieces], *extra)


def assembled(values, axis):
    size = lax.axis_size(axis)
    if size != 2:
        return lax.all_gather(values, axis, axis=1, tiled=True)
    other = swap(values, axis, 1)
    first = lax.axis_index(axis) == 0
    return jnp.concatenate(
        [jnp.where(first, values, other), jnp.where(first, other, values)], axis=1
    )


def halve(values, axis, bit):
    mine = (lax.axis_index(axis) // bit) % 2
    keep = lax.dynamic_index_in_dim(values, mine, 0, keepdims=False)
    give = lax.dynamic_index_in_dim(values, 1 - mine, 0, keepdims=False)
    return keep + swap(give, axis, bit)


def scatter_sum(values, axis):
    size = lax.axis_size(axis)
    if size & (size - 1):
        return lax.psum_scatter(values, axis, scatter_dimension=0, tiled=False)
    bit = 1
    while bit < size:
        paired = values.reshape((-1, 2) + values.shape[1:])
        values = halve(jnp.moveaxis(paired, 1, 0), axis, bit)
        bit *= 2
    return values[0]


def row_sum(values, axis, columns):
    size = lax.axis_size(axis)
    if size & (size - 1) or size < 2:
        return [assembled(lax.psum(values, axis), columns)]
    part = halve(values.reshape((2, -1) + values.shape[1:]), axis, 1)
    bit = 2
    while bit < size:
        part = part + swap(part, axis, bit)
        bit *= 2
    if lax.axis_size(columns) == 2:
        beside = swap(part, columns, 1)
        return [part, beside, swap(part, axis, 1), swap(beside, axis, 1)]
    part = assembled(part, columns)
    other = swap(part, axis, 1)
    even = lax.axis_index(axis) % 2 == 0
    return [jnp.concatenate([jnp.where(even, part, other), jnp.where(even, other, part)], axis=0)]


def body(
    diag_two,
    diag_one,
    cross_tile,
    left_two,
    left_one,
    below_left,
    panel_two,
    panel_one,
    grad_diag_two,
    grad_diag_one,
    grad_cross,
    grad_left_two,
    grad_left_one,
    grad_below,
    grad_panel_two,
    grad_panel_one,
):
    size = diag_two.shape[0]
    share = grad_left_two.shape[0]
    width = panel_two.shape[1]
    row_start = lax.axis_index("row") * share
    col_start = lax.axis_index("col") * width
    cube = 2 * size**3

    pieces_two = gathered(grad_panel_two, "col")
    pieces_one = gathered(grad_panel_one, "col")
    inv_two, inv_one, cross_inv = local_call(
        invert_kernel, (diag_two, diag_one, cross_tile), 3, 60 * cube
    )
    solved_two, *own_two = solve(pieces_two, inv_two)
    solved_one, *own_one = solve(pieces_one, inv_one, solved_two, cross_inv)
    place = jnp.stack([lax.axis_index("col"), lax.axis_index("row") % 2]).astype(jnp.int32)
    partial = jnp.concatenate(
        [
            large(solved_two, panel_two, (0, 0)),
            large(solved_two, panel_one, (0, 0)),
            large(solved_one, panel_one, (0, 0)),
        ],
        axis=0,
    )
    grams = row_sum(partial, "row", "col")
    rows = lax.axis_size("row")
    lefts = jnp.stack(
        [
            large(solved_two, below_left, (0, 0)).reshape(rows, share, -1),
            large(solved_one, below_left, (0, 0)).reshape(rows, share, -1),
        ],
        axis=1,
    )
    summed = scatter_sum(lefts, "row")
    out_below = (
        grad_below - large(solved_two, left_two, (1, 0)) - large(solved_one, left_one, (1, 0))
    )
    sym_two, sym_one, half_two, half_one, out_cross = local_call(
        chain_kernel,
        (
            diag_two,
            diag_one,
            cross_tile,
            inv_two,
            inv_one,
            grad_diag_two,
            grad_diag_one,
            grad_cross,
            place,
            *grams,
        ),
        5,
        60 * cube,
    )
    sym_two_rows = lax.dynamic_slice_in_dim(sym_two, row_start, share, 0)
    sym_one_rows = lax.dynamic_slice_in_dim(sym_one, row_start, share, 0)
    cross_rows = lax.dynamic_slice_in_dim(out_cross, row_start, share, 0)
    cross_cols = lax.dynamic_slice_in_dim(out_cross, row_start, share, 1)
    out_left_two = (
        grad_left_two
        - summed[0]
        - large(sym_two_rows, left_two, (1, 0))
        - large(cross_rows, left_one, (1, 0))
    )
    out_left_one = (
        grad_left_one
        - summed[1]
        - large(cross_cols, left_two, (0, 0))
        - large(sym_one_rows, left_one, (1, 0))
    )
    return (
        out_below,
        out_left_two,
        out_left_one,
        half_two,
        half_one,
        out_cross,
        own_two[0] if own_two else lax.dynamic_slice_in_dim(solved_two, col_start, width, 1),
        own_one[0] if own_one else lax.dynamic_slice_in_dim(solved_one, col_start, width, 1),
    )


MESH = pl.DeviceIdType.MESH


def split(values):
    high = values.astype(jnp.bfloat16)
    return high, (values - high.astype(jnp.float32)).astype(jnp.bfloat16)


def thrice(left, right, contract=(1, 0)):
    def single(one, other):
        return lax.dot_general(
            one,
            other,
            ((contract[:1], contract[1:]), ((), ())),
            preferred_element_type=jnp.float32,
        )

    return (single(left[1], right[0]) + single(left[0], right[1])) + single(left[0], right[0])


def fused_kernel(plan, *refs):
    (
        two_hbm,
        one_hbm,
        cross_hbm,
        left_two_hbm,
        left_one_hbm,
        below_hbm,
        panel_two_hbm,
        panel_one_hbm,
        grad_two_hbm,
        grad_one_hbm,
        grad_cross_hbm,
        grad_left_two_hbm,
        grad_left_one_hbm,
        grad_below_hbm,
        grad_panel_two_hbm,
        grad_panel_one_hbm,
    ) = refs[:16]
    (
        acc,
        panel_out,
        half_two,
        next_cross,
        middle_one,
        inverse_one,
        grad_left,
        left_high,
        left_low,
    ) = refs[16:25]
    (
        two,
        one,
        cross,
        left,
        below,
        panels,
        grad_two,
        grad_one,
        grad_cross,
        full_two,
        full_one,
        solved_high,
        solved_low,
        below_high,
        below_low,
        inverse_two,
        crossed,
        pre,
        partial,
        from_core,
        chip,
        from_x,
        own,
        oth,
        lefts,
        lefts_core,
        lefts_send,
        lefts_x,
        sym_two,
        cross_t,
        load_sem,
        y_send,
        y_recv,
        z_send,
        z_recv,
        w_send,
        w_recv,
        l_send,
        l_recv,
    ) = refs[25:]
    size = two.shape[0]
    rows, width = grad_panel_two_hbm.shape
    share = grad_left.shape[1]
    quarter = width // 2
    at_row, at_col, at_depth = (lax.axis_index(name) for name in ("row", "col", "depth"))
    core = lax.rem(at_row, 2)
    side = lax.div(at_row, 2)
    first = at_col == 0
    part = lax.rem(at_depth, 2)
    to_core = (at_row + 1 - 2 * core, at_col, at_depth)
    to_x = (at_row + 2 - 4 * side, at_col, at_depth)
    to_y = (at_row, 1 - at_col, at_depth)
    to_z = (at_row, at_col, at_depth + 1 - 2 * part)

    loads = []

    def load(source, target):
        copy = pltpu.make_async_copy(source, target, load_sem.at[len(loads)])
        copy.start()
        loads.append(copy)
        return copy

    own_two = load(grad_panel_two_hbm, full_two.at[:, :width])
    pan_two = load(panel_two_hbm, panels.at[:, :width])
    pan_one = load(panel_one_hbm, panels.at[:, width:])
    own_one = load(grad_panel_one_hbm, full_one.at[:, :width])
    block_loads = [load(two_hbm, two), load(one_hbm, one)]
    small_loads = [
        load(cross_hbm, cross),
        load(grad_two_hbm, grad_two),
        load(grad_one_hbm, grad_one),
        load(grad_cross_hbm, grad_cross),
    ]
    below_load = load(below_hbm, below)
    left_loads = [load(left_two_hbm, left.at[:size]), load(left_one_hbm, left.at[size:])]
    acc_load = load(grad_below_hbm, acc)
    grad_left_loads = [
        load(grad_left_two_hbm, grad_left.at[0]),
        load(grad_left_one_hbm, grad_left.at[1]),
    ]

    barrier = pltpu.get_barrier_semaphore()
    for target in (to_core, to_x, to_y, to_z):
        pl.semaphore_signal(barrier, inc=1, device_id=target, device_id_type=MESH)
    pl.semaphore_wait(barrier, 4)

    sends = []

    def send(source, target, sems, at, device):
        copy = pltpu.make_async_remote_copy(
            src_ref=source,
            dst_ref=target,
            send_sem=sems[0].at[at],
            recv_sem=sems[1].at[at],
            device_id=device,
            device_id_type=MESH,
        )
        copy.start()
        sends.append(copy)
        return copy

    fulls = (full_two, full_one)
    y_copies = []
    places = []
    for panel, source in enumerate((grad_panel_two_hbm, grad_panel_one_hbm)):
        forwarded, direct = plan[panel]
        extent = sum(forwarded)
        begin = 0
        for at, count in enumerate(forwarded + direct):
            if at == len(forwarded):
                begin = 2 * extent
            start = part * extent + begin if at < len(forwarded) else begin
            place = pl.ds(pl.multiple_of(start, 8), count)
            begin += count
            at = len(y_copies)
            y_copies.append(
                send(source.at[place, :], fulls[panel].at[place, width:], (y_send, y_recv), at, to_y)
            )
            places.append((panel, place))
    order = list(range(len(plan[0][0]))) + [
        len(plan[0][0]) + len(plan[0][1]) + at for at in range(len(plan[1][0]))
    ]
    z_copies = []

    def forward():
        at = order[len(z_copies)]
        y_copies[at].wait_recv()
        panel, place = places[at]
        piece = fulls[panel].at[place, width:]
        z_copies.append(send(piece, piece, (z_send, z_recv), len(z_copies), to_z))

    mine = pl.ds(pl.multiple_of(core * quarter, quarter), quarter)
    theirs = pl.ds(pl.multiple_of((1 - core) * quarter, quarter), quarter)
    stages = ((0, 3), (3, 2), (5, 1))
    waits = {}

    def w_core(stage):
        start, count = stages[stage]
        blocks = pl.ds(start, count)
        waits["core", stage] = send(
            partial.at[blocks, theirs, :],
            from_core.at[blocks],
            (w_send, w_recv),
            stage * 5,
            to_core,
        )

    def w_x(stage):
        start, count = stages[stage]
        blocks = pl.ds(start, count)
        waits["core", stage].wait_recv()
        chip[blocks] = partial[blocks, mine, :] + from_core[blocks]
        waits["x", stage] = send(
            chip.at[blocks], from_x.at[blocks], (w_send, w_recv), stage * 5 + 1, to_x
        )

    def w_y(stage):
        start, count = stages[stage]
        blocks = pl.ds(start, count)
        waits["x", stage].wait_recv()
        own[blocks, mine, :] = chip[blocks] + from_x[blocks]
        piece = own.at[blocks, mine, :]
        waits["y", stage] = send(
            piece, oth.at[blocks, mine, :], (w_send, w_recv), stage * 5 + 2, to_y
        )
        waits["own", stage] = send(piece, piece, (w_send, w_recv), stage * 5 + 3, to_core)

    def w_last(stage):
        start, count = stages[stage]
        blocks = pl.ds(start, count)
        waits["y", stage].wait_recv()
        piece = oth.at[blocks, mine, :]
        waits["oth", stage] = send(piece, piece, (w_send, w_recv), stage * 5 + 4, to_core)

    def w_done(stage):
        waits["own", stage].wait_recv()
        waits["oth", stage].wait_recv()

    def joined_at(diagonal, off):
        near, far = own[diagonal], oth[diagonal]
        near_off, far_off = own[off], oth[off]
        top = [jnp.where(first, near, far), jnp.where(first, far_off, near_off)]
        bottom = [jnp.where(first, near_off, far_off), jnp.where(first, far, near)]
        return jnp.concatenate(
            [jnp.concatenate(top, axis=1), jnp.concatenate(bottom, axis=1)], axis=0
        )

    own_two.wait()
    pan_two.wait()
    pan_one.wait()
    panel_parts = split(panels[...])
    found = thrice(split(full_two[:, :width]), panel_parts, (0, 0))
    partial[0] = found[:, :width]
    partial[1] = found[:, width:]
    own_one.wait()
    partial[2] = thrice(
        split(full_one[:, :width]), tuple(piece[:, width:] for piece in panel_parts), (0, 0)
    )
    w_core(0)

    for copy in block_loads:
        copy.wait()
    grid_rows, grid_cols = grid_of(size)
    scale = jnp.where(
        grid_rows > grid_cols, 1.0, jnp.where(grid_rows == grid_cols, 0.5, 0.0)
    )
    events = {
        1: lambda: w_x(0),
        2: forward,
        4: forward,
        6: lambda: (forward(), w_y(0)),
    }
    mid = size // 2
    blocks = []
    for ref in (two, one):
        blocks += [ref[:mid, :mid], ref[mid:, mid:]]
    found = invert_steps(blocks, events)
    for at, (ref, inverse) in enumerate(((two, inverse_two), (one, inverse_one))):
        step_product = small(ref[mid:, :mid], found[2 * at])
        inverse[:mid, :mid] = found[2 * at]
        inverse[mid:, mid:] = found[2 * at + 1]
        inverse[:mid, mid:] = jnp.zeros((mid, size - mid), jnp.float32)
        inverse[mid:, :mid] = -small(found[2 * at + 1], step_product)
    forward()

    def local_rows(values):
        near = jnp.where(first, values[:width, :], values[width:, :])
        away = jnp.where(first, values[width:, :], values[:width, :])
        return jnp.concatenate([near, away], axis=0)

    def own_columns(values):
        return jnp.where(first, values[:, :width], values[:, width:])

    right_two = split(local_rows(inverse_two[...]))

    def solve_two(begin, count):
        place = pl.ds(pl.multiple_of(begin, 8), count)
        pieces = split(full_two[place, :])
        off = thrice(
            tuple(piece[:, width:] for piece in pieces), split(panels[place, :]), (0, 0)
        )
        total = thrice(pieces, right_two)
        panel_out[0, place, :] = own_columns(total)
        high, low = split(total)
        solved_high[place, :size] = high
        solved_low[place, :size] = low
        return off

    half = rows // 2
    off_near = solve_two(part * half, half)
    for copy in small_loads:
        copy.wait()
    split_cross = split(cross[...])
    split_two = split(inverse_two[...])
    split_one = split(inverse_one[...])
    crossed_one = thrice(split_cross, split_one)
    crossed[...] = thrice(split_two, split_cross)
    forward()
    pre[0] = thrice(split(two[...]), split(grad_two[...]), (0, 0))
    pre[1] = thrice(split(one[...]), split(grad_one[...]), (0, 0))
    right_one = split(jnp.concatenate([local_rows(inverse_one[...]), -crossed_one], axis=0))
    below_load.wait()
    high, low = split(below[...])
    below_high[...] = high
    below_low[...] = low
    forward()
    for at in range(len(plan[0][0])):
        z_copies[at].wait_recv()
    off_far = solve_two((1 - part) * half, half)
    off = off_near + off_far
    partial[3] = off[:, :width]
    partial[4] = off[:, width:]
    w_core(1)
    forward()
    for copy in left_loads:
        copy.wait()
    high, low = split(left[...])
    left_high[...] = high
    left_low[...] = low
    forward()
    w_x(1)
    l_waits = {}

    def lefts_of(panel):
        columns = pl.ds(panel * size, size)
        product_of = thrice(
            (solved_high[:, columns], solved_low[:, columns]),
            (below_high[...], below_low[...]),
            (0, 0),
        )
        lefts[panel] = product_of.reshape(lefts.shape[1:])
        for at in range(2):
            l_waits["core", panel, at] = send(
                lefts.at[panel, at, 1 - core],
                lefts_core.at[panel, at],
                (l_send, l_recv),
                panel * 3 + at,
                to_core,
            )

    def lefts_away(panel):
        for at in range(2):
            l_waits["core", panel, at].wait_recv()
        lefts_send[panel] = lefts[panel, 1 - side, core] + lefts_core[panel, 1 - side]
        l_waits["x", panel] = send(
            lefts_send.at[panel], lefts_x.at[panel], (l_send, l_recv), panel * 3 + 2, to_x
        )

    def lefts_end(panel):
        l_waits["x", panel].wait_recv()
        return (lefts[panel, side, core] + lefts_core[panel, side]) + lefts_x[panel]

    tiles = 4
    tile = rows // tiles

    def below_of(panel, at):
        columns = pl.ds(panel * size, size)
        place = pl.ds(at * tile, tile)
        acc[place, :] = acc[place, :] - thrice(
            (solved_high[place, columns], solved_low[place, columns]),
            (left_high[columns, :], left_low[columns, :]),
        )

    def solve_one(begin, count):
        place = pl.ds(pl.multiple_of(begin, 8), count)
        pieces = split(full_one[place, :])
        off = thrice(
            tuple(piece[:, width:] for piece in pieces), split(panels[place, width:]), (0, 0)
        )
        both = tuple(
            jnp.concatenate([piece, before[place, :size]], axis=1)
            for piece, before in zip(pieces, (solved_high, solved_low))
        )
        total = thrice(both, right_one)
        panel_out[1, place, :] = own_columns(total)
        high, low = split(total)
        solved_high[place, size:] = high
        solved_low[place, size:] = low
        return off

    lefts_of(0)
    extent = sum(plan[1][0])
    off_near = solve_one(part * extent, extent)
    w_y(1)
    lefts_away(0)
    for at in range(len(plan[0][0]), len(order)):
        z_copies[at].wait_recv()
    off_far = solve_one((1 - part) * extent, extent)
    off = off_near + off_far
    if plan[1][1]:
        for at in range(len(plan[1][1])):
            y_copies[len(y_copies) - 1 - at].wait_recv()
        off = off + solve_one(2 * extent, sum(plan[1][1]))
    partial[5] = off
    w_core(2)
    lefts_of(1)
    w_x(2)
    w_last(0)
    acc_load.wait()
    below_of(0, 0)
    lefts_away(1)
    below_of(0, 1)
    below_of(0, 2)
    w_y(2)
    w_last(1)
    below_of(0, 3)
    w_done(0)
    w_done(1)

    inner = scale * (pre[0] - joined_at(0, 3))
    middle = split(inner + inner.T)
    cross_gram = thrice(split_two, split(joined_at(1, 4)), (0, 0))
    spread = thrice(
        split_two,
        split(
            thrice(
                middle, split(jnp.concatenate([inverse_two[...], crossed[...]], axis=1))
            )
        ),
        (0, 0),
    )
    sym_two[...] = spread[:, :size]
    half_two[...] = scale * spread[:, :size]
    following = split(grad_cross[...] - cross_gram - spread[:, size:])
    found = thrice(following, split_one)
    next_cross[...] = found
    cross_t[...] = found.T
    ready = pre[1] - (
        thrice(following, split_cross, (0, 0)) - thrice(split_cross, split(cross_gram), (0, 0))
    )
    for at in range(tiles):
        below_of(1, at)
    w_last(2)
    mine_rows = pl.ds(pl.multiple_of(at_row * share, share), share)
    for copy in grad_left_loads:
        copy.wait()
    head = split(jnp.concatenate([sym_two[mine_rows, :], next_cross[mine_rows, :]], axis=1))
    grad_left[0] = (grad_left[0] - lefts_end(0)) - thrice(
        head, (left_high[...], left_low[...])
    )
    grad_left[1] = (grad_left[1] - lefts_end(1)) - thrice(
        split(cross_t[mine_rows, :]), (left_high[:size], left_low[:size])
    )
    w_done(2)
    inner = scale * (ready - joined_at(2, 5))
    middle_one[...] = inner + inner.T
    for copy in sends:
        copy.wait_send()


def tail_kernel(*refs):
    (
        acc,
        panel_out,
        half_two,
        next_cross,
        middle_one,
        inverse_one,
        grad_left,
        left_high,
        left_low,
    ) = refs[:9]
    (
        out_below,
        out_left_two,
        out_left_one,
        out_diag_two,
        out_diag_one,
        out_cross,
        out_panel_two,
        out_panel_one,
    ) = refs[9:17]
    sym_one, half_one, last, store_sem = refs[17:]
    size = sym_one.shape[0]
    share = last.shape[0]
    stores = []

    def store(source, target):
        copy = pltpu.make_async_copy(source, target, store_sem.at[len(stores)])
        copy.start()
        stores.append(copy)

    store(acc, out_below)
    store(panel_out.at[0], out_panel_two)
    store(panel_out.at[1], out_panel_one)
    store(half_two, out_diag_two)
    store(next_cross, out_cross)
    store(grad_left.at[0], out_left_two)
    inverse = split(inverse_one[...])
    found = thrice(inverse, split(thrice(split(middle_one[...]), inverse)), (0, 0))
    sym_one[...] = found
    rows, cols = grid_of(size)
    half_one[...] = jnp.where(rows > cols, found, jnp.where(rows == cols, 0.5 * found, 0.0))
    store(half_one, out_diag_one)
    mine_rows = pl.ds(pl.multiple_of(lax.axis_index("row") * share, share), share)
    last[...] = grad_left[1] - thrice(
        split(sym_one[mine_rows, :]), (left_high[size:, :], left_low[size:, :])
    )
    store(last, out_left_one)
    for copy in stores:
        copy.wait()


def invert_steps(blocks, events):
    size = blocks[0].shape[0]
    rows, cols = grid_of(size)
    apart = rows ^ cols
    lower = rows > cols
    inverses = []
    for block in blocks:
        diagonal = jnp.where(rows == cols, block, 0.0)
        down = 1.0 / jnp.sum(diagonal, axis=1, keepdims=True)
        across = 1.0 / jnp.sum(diagonal, axis=0, keepdims=True)
        pair = jnp.where(lower & (apart == 1), block, 0.0)
        inverses.append(jnp.where(rows == cols, down, 0.0) - pair * down * across)
    level = 1
    while (2 << level) <= size:
        mask = lower & ((apart >> level) == 1)
        steps = [
            small(jnp.where(mask, block, 0.0), inverse) for block, inverse in zip(blocks, inverses)
        ]
        inverses = [inverse - small(inverse, step) for inverse, step in zip(inverses, steps)]
        if level in events:
            events[level]()
        level += 1
    for late in sorted(events):
        if late >= level:
            events[late]()
    return inverses


def fused(*arrays):
    two, left, below, grad_left = arrays[0], arrays[3], arrays[5], arrays[11]
    size = two.shape[0]
    rows, width = arrays[14].shape
    columns = below.shape[1]
    share = grad_left.shape[0]
    quarter = width // 2
    piece = rows // 8
    plan = (
        ([piece] * 4, []),
        ([piece] * 2 + [piece // 2] * 2, [piece] * 2),
    )
    y_count = sum(len(go) + len(stay) for go, stay in plan)
    z_count = sum(len(go) for go, _ in plan)

    def real(*shape):
        return pltpu.VMEM(shape, jnp.float32)

    def short(*shape):
        return pltpu.VMEM(shape, jnp.bfloat16)

    def outs(*shape):
        return jax.ShapeDtypeStruct(shape, jnp.float32)

    scratch = [
        real(size, size),
        real(size, size),
        real(size, size),
        real(2 * size, columns),
        real(rows, columns),
        real(rows, size),
        real(size, size),
        real(size, size),
        real(size, size),
        real(rows, size),
        real(rows, size),
        short(rows, 2 * size),
        short(rows, 2 * size),
        short(rows, columns),
        short(rows, columns),
        real(size, size),
        real(size, size),
        real(2, size, size),
        real(6, width, width),
        real(6, quarter, width),
        real(6, quarter, width),
        real(6, quarter, width),
        real(6, width, width),
        real(6, width, width),
        real(2, 2, 2, share, columns),
        real(2, 2, share, columns),
        real(2, share, columns),
        real(2, share, columns),
        real(size, size),
        real(size, size),
        pltpu.SemaphoreType.DMA((16,)),
        pltpu.SemaphoreType.DMA((y_count,)),
        pltpu.SemaphoreType.DMA((y_count,)),
        pltpu.SemaphoreType.DMA((z_count,)),
        pltpu.SemaphoreType.DMA((z_count,)),
        pltpu.SemaphoreType.DMA((15,)),
        pltpu.SemaphoreType.DMA((15,)),
        pltpu.SemaphoreType.DMA((6,)),
        pltpu.SemaphoreType.DMA((6,)),
    ]
    anywhere = pl.BlockSpec(memory_space=pl.ANY)
    near = pl.BlockSpec(memory_space=pltpu.VMEM)
    far = pl.BlockSpec(memory_space=pltpu.HBM)
    kept = pl.pallas_call(
        lambda *refs: fused_kernel(plan, *refs),
        out_shape=[
            real(rows, columns),
            real(2, rows, width),
            real(size, size),
            real(size, size),
            real(size, size),
            real(size, size),
            real(2, share, columns),
            short(2 * size, columns),
            short(2 * size, columns),
        ],
        in_specs=[far] * 16,
        out_specs=[near] * 9,
        scratch_shapes=scratch,
        compiler_params=pltpu.CompilerParams(
            collective_id=0, has_side_effects=True, vmem_limit_bytes=40 << 20
        ),
        cost_estimate=pl.CostEstimate(
            flops=24 * rows * size * columns, bytes_accessed=16 * rows * columns, transcendentals=0
        ),
    )(*[pltpu.with_memory_space_constraint(values, pltpu.HBM) for values in arrays])
    return pl.pallas_call(
        tail_kernel,
        out_shape=[
            outs(rows, columns),
            outs(share, columns),
            outs(share, columns),
            outs(size, size),
            outs(size, size),
            outs(size, size),
            outs(rows, width),
            outs(rows, width),
        ],
        in_specs=[near] * 9,
        out_specs=[anywhere] * 8,
        scratch_shapes=[
            real(size, size),
            real(size, size),
            real(share, columns),
            pltpu.SemaphoreType.DMA((8,)),
        ],
        compiler_params=pltpu.CompilerParams(vmem_limit_bytes=8 << 20),
        cost_estimate=pl.CostEstimate(
            flops=12 * size**3, bytes_accessed=8 * rows * columns, transcendentals=0
        ),
    )(*[pltpu.with_memory_space_constraint(values, pltpu.VMEM) for values in kept])


def fits(mesh):
    return mesh.shape["row"] == 4 and mesh.shape["col"] == 2 and mesh.shape["depth"] % 2 == 0


def solution(mesh):
    panels = P("row", "col")
    lefts = P(None, ("col", "depth"))
    blocks = P("row", ("col", "depth"))
    return jax.shard_map(
        fused if fits(mesh) else body,
        mesh=mesh,
        in_specs=(P(), P(), P(), lefts, lefts, blocks, panels, panels)
        + (P(), P(), P(), blocks, blocks, blocks, panels, panels),
        out_specs=(blocks, blocks, blocks, P(), P(), P(), panels, panels),
        check_vma=False,
    )
```

```python
import jax
import jax.numpy as jnp
from jax import lax
from jax.experimental import pallas as pl
from jax.experimental.pallas import tpu as pltpu
from jax.sharding import PartitionSpec as P


def large(left, right, contract):
    return lax.dot_general(
        left,
        right,
        ((contract[:1], contract[1:]), ((), ())),
        precision=lax.Precision.HIGH,
        preferred_element_type=jnp.float32,
    )


def small(left, right, contract=(1, 0)):
    return lax.dot_general(
        left,
        right,
        ((contract[:1], contract[1:]), ((), ())),
        precision=lax.Precision.HIGHEST,
        preferred_element_type=jnp.float32,
    )


def grid_of(size):
    rows = lax.broadcasted_iota(jnp.int32, (size, size), 0)
    cols = lax.broadcasted_iota(jnp.int32, (size, size), 1)
    return rows, cols


def invert_all(blocks):
    size = blocks[0].shape[0]
    rows, cols = grid_of(size)
    apart = rows ^ cols
    lower = rows > cols
    inverses = []
    for block in blocks:
        diagonal = jnp.where(rows == cols, block, 0.0)
        down = 1.0 / jnp.sum(diagonal, axis=1, keepdims=True)
        across = 1.0 / jnp.sum(diagonal, axis=0, keepdims=True)
        pair = jnp.where(lower & (apart == 1), block, 0.0)
        inverses.append(jnp.where(rows == cols, down, 0.0) - pair * down * across)
    level = 1
    while (2 << level) <= size:
        mask = lower & ((apart >> level) == 1)
        steps = [
            small(jnp.where(mask, block, 0.0), inverse) for block, inverse in zip(blocks, inverses)
        ]
        inverses = [inverse - small(inverse, step) for inverse, step in zip(inverses, steps)]
        level += 1
    return inverses


def invert_kernel(two_ref, one_ref, cross_ref, inv_two_ref, inv_one_ref, cross_inv_ref):
    half = two_ref.shape[0] // 2
    refs = (two_ref, one_ref)
    outs = (inv_two_ref, inv_one_ref)
    blocks = []
    for ref in refs:
        blocks += [ref[:half, :half], ref[half:, half:]]
    inverses = invert_all(blocks)
    steps = [small(ref[half:, :half], inverses[2 * at]) for at, ref in enumerate(refs)]
    for at, out in enumerate(outs):
        out[:half, :half] = inverses[2 * at]
        out[half:, half:] = inverses[2 * at + 1]
        out[:half, half:] = jnp.zeros((half, half), jnp.float32)
        out[half:, :half] = -small(inverses[2 * at + 1], steps[at])
    cross_inv_ref[...] = small(cross_ref[...], inv_one_ref[...])


def chain_kernel(
    two_ref,
    one_ref,
    cross_ref,
    inv_two_ref,
    inv_one_ref,
    grad_two_ref,
    grad_one_ref,
    grad_cross_ref,
    place_ref,
    *rest,
):
    grams, outs = rest[:-5], rest[-5:]
    chain(
        two_ref,
        one_ref,
        cross_ref,
        inv_two_ref,
        inv_one_ref,
        grad_two_ref,
        grad_one_ref,
        grad_cross_ref,
        joined(grams, place_ref),
        *outs,
    )


def joined(grams, place_ref):
    if len(grams) == 1:
        return grams[0][...]
    mine, beside, twin, across = [gram[...] for gram in grams]
    left = place_ref[0] == 0
    upper = place_ref[1] == 0
    own = jnp.concatenate([jnp.where(left, mine, beside), jnp.where(left, beside, mine)], axis=1)
    far = jnp.concatenate([jnp.where(left, twin, across), jnp.where(left, across, twin)], axis=1)
    return jnp.concatenate([jnp.where(upper, own, far), jnp.where(upper, far, own)], axis=0)


def chain(
    two_ref,
    one_ref,
    cross_ref,
    inv_two_ref,
    inv_one_ref,
    grad_two_ref,
    grad_one_ref,
    grad_cross_ref,
    grams,
    sym_two_ref,
    sym_one_ref,
    half_two_ref,
    half_one_ref,
    out_cross_ref,
):
    size = two_ref.shape[0]
    rows, cols = grid_of(size)
    lower = rows >= cols
    scale = jnp.where(rows > cols, 1.0, jnp.where(rows == cols, 0.5, 0.0))

    def sym(factor, inverse, cotangent):
        inner = scale * small(factor, cotangent, (0, 0))
        spread = small(small(inverse, inner, (0, 0)), inverse)
        return spread + spread.T

    gram_two = grams[:size, :]
    gram_cross = grams[size : 2 * size, :]
    gram_below = grams[2 * size :, :]
    sym_two = sym(
        two_ref[...], inv_two_ref[...], grad_two_ref[...] - jnp.where(lower, gram_two, 0.0)
    )
    sym_two_ref[...] = sym_two
    half_two_ref[...] = scale * sym_two
    cross_next = grad_cross_ref[...] - gram_cross - small(sym_two, cross_ref[...])
    out_cross = small(cross_next, inv_one_ref[...])
    out_cross_ref[...] = out_cross
    gram_one = small(out_cross, cross_ref[...], (0, 0)) + gram_below
    sym_one = sym(
        one_ref[...], inv_one_ref[...], grad_one_ref[...] - jnp.where(lower, gram_one, 0.0)
    )
    sym_one_ref[...] = sym_one
    half_one_ref[...] = scale * sym_one


def local_call(kernel, operands, count, flops):
    size = operands[0].shape[0]
    moved = 4 * size * size * (len(operands) + count)
    return pl.pallas_call(
        kernel,
        out_shape=[jax.ShapeDtypeStruct((size, size), jnp.float32)] * count,
        in_specs=[
            pl.BlockSpec(memory_space=pltpu.SMEM if operand.ndim == 1 else pltpu.VMEM)
            for operand in operands
        ],
        out_specs=[pl.BlockSpec(memory_space=pltpu.VMEM)] * count,
        cost_estimate=pl.CostEstimate(flops=flops, bytes_accessed=moved, transcendentals=0),
    )(*operands)


def swap(values, axis, bit):
    size = lax.axis_size(axis)
    return lax.ppermute(values, axis, [(at, at ^ bit) for at in range(size)])


def gathered(values, axis):
    if lax.axis_size(axis) != 2:
        return [(lax.all_gather(values, axis, axis=1, tiled=True), 0)]
    width = values.shape[1]
    at = lax.axis_index(axis)
    return [(values, at * width), (swap(values, axis, 1), (1 - at) * width)]


def parted(values):
    high = values.astype(jnp.bfloat16)
    return high, (values - high.astype(jnp.float32)).astype(jnp.bfloat16)


def product(left, right):
    (left_high, left_low), (right_high, right_low) = parted(left), parted(right)

    def single(one, other):
        return jnp.dot(one, other, preferred_element_type=jnp.float32)

    return (single(left_low, right_high) + single(left_high, right_low)) + single(
        left_high, right_high
    )


def solve_kernel(count, starts_ref, inverse_ref, *refs):
    pieces, extra, outs = refs[:count], refs[count:-count], refs[-count:]
    total = None
    for at, piece in enumerate(pieces):
        width = piece.shape[1]
        rows = inverse_ref[pl.ds(pl.multiple_of(starts_ref[at], width), width), :]
        part = product(piece[...], rows)
        total = part if total is None else total + part
    if extra:
        total = total - product(extra[0][...], extra[1][...])
    outs[0][...] = total
    if count > 1:
        width = outs[1].shape[1]
        outs[1][...] = jnp.where(starts_ref[0] == 0, total[:, :width], total[:, width:])


def solve(pieces, inverse, *extra):
    count = len(pieces)
    rows, width = pieces[0][0].shape
    size = inverse.shape[0]
    block = rows // 4
    starts = jnp.stack([jnp.asarray(start, jnp.int32) for _, start in pieces])

    def tall(columns):
        return pl.BlockSpec((block, columns), lambda step: (step, 0))

    whole = pl.BlockSpec((size, size), lambda step: (0, 0))
    widths = [size, width][:count]
    return pl.pallas_call(
        lambda *refs: solve_kernel(count, *refs),
        grid=(4,),
        out_shape=[jax.ShapeDtypeStruct((rows, columns), jnp.float32) for columns in widths],
        in_specs=[pl.BlockSpec(memory_space=pltpu.SMEM), whole]
        + [tall(values.shape[1]) for values, _ in pieces]
        + ([tall(size), whole] if extra else []),
        out_specs=[tall(columns) for columns in widths],
        cost_estimate=pl.CostEstimate(
            flops=6 * rows * size * size, bytes_accessed=12 * rows * size, transcendentals=0
        ),
    )(starts, inverse, *[values for values, _ in pieces], *extra)


def assembled(values, axis):
    size = lax.axis_size(axis)
    if size != 2:
        return lax.all_gather(values, axis, axis=1, tiled=True)
    other = swap(values, axis, 1)
    first = lax.axis_index(axis) == 0
    return jnp.concatenate(
        [jnp.where(first, values, other), jnp.where(first, other, values)], axis=1
    )


def halve(values, axis, bit):
    mine = (lax.axis_index(axis) // bit) % 2
    keep = lax.dynamic_index_in_dim(values, mine, 0, keepdims=False)
    give = lax.dynamic_index_in_dim(values, 1 - mine, 0, keepdims=False)
    return keep + swap(give, axis, bit)


def scatter_sum(values, axis):
    size = lax.axis_size(axis)
    if size & (size - 1):
        return lax.psum_scatter(values, axis, scatter_dimension=0, tiled=False)
    bit = 1
    while bit < size:
        paired = values.reshape((-1, 2) + values.shape[1:])
        values = halve(jnp.moveaxis(paired, 1, 0), axis, bit)
        bit *= 2
    return values[0]


def row_sum(values, axis, columns):
    size = lax.axis_size(axis)
    if size & (size - 1) or size < 2:
        return [assembled(lax.psum(values, axis), columns)]
    part = halve(values.reshape((2, -1) + values.shape[1:]), axis, 1)
    bit = 2
    while bit < size:
        part = part + swap(part, axis, bit)
        bit *= 2
    if lax.axis_size(columns) == 2:
        beside = swap(part, columns, 1)
        return [part, beside, swap(part, axis, 1), swap(beside, axis, 1)]
    part = assembled(part, columns)
    other = swap(part, axis, 1)
    even = lax.axis_index(axis) % 2 == 0
    return [jnp.concatenate([jnp.where(even, part, other), jnp.where(even, other, part)], axis=0)]


def body(
    diag_two,
    diag_one,
    cross_tile,
    left_two,
    left_one,
    below_left,
    panel_two,
    panel_one,
    grad_diag_two,
    grad_diag_one,
    grad_cross,
    grad_left_two,
    grad_left_one,
    grad_below,
    grad_panel_two,
    grad_panel_one,
):
    size = diag_two.shape[0]
    share = grad_left_two.shape[0]
    width = panel_two.shape[1]
    row_start = lax.axis_index("row") * share
    col_start = lax.axis_index("col") * width
    cube = 2 * size**3

    pieces_two = gathered(grad_panel_two, "col")
    pieces_one = gathered(grad_panel_one, "col")
    inv_two, inv_one, cross_inv = local_call(
        invert_kernel, (diag_two, diag_one, cross_tile), 3, 60 * cube
    )
    solved_two, *own_two = solve(pieces_two, inv_two)
    solved_one, *own_one = solve(pieces_one, inv_one, solved_two, cross_inv)
    place = jnp.stack([lax.axis_index("col"), lax.axis_index("row") % 2]).astype(jnp.int32)
    partial = jnp.concatenate(
        [
            large(solved_two, panel_two, (0, 0)),
            large(solved_two, panel_one, (0, 0)),
            large(solved_one, panel_one, (0, 0)),
        ],
        axis=0,
    )
    grams = row_sum(partial, "row", "col")
    rows = lax.axis_size("row")
    lefts = jnp.stack(
        [
            large(solved_two, below_left, (0, 0)).reshape(rows, share, -1),
            large(solved_one, below_left, (0, 0)).reshape(rows, share, -1),
        ],
        axis=1,
    )
    summed = scatter_sum(lefts, "row")
    out_below = (
        grad_below - large(solved_two, left_two, (1, 0)) - large(solved_one, left_one, (1, 0))
    )
    sym_two, sym_one, half_two, half_one, out_cross = local_call(
        chain_kernel,
        (
            diag_two,
            diag_one,
            cross_tile,
            inv_two,
            inv_one,
            grad_diag_two,
            grad_diag_one,
            grad_cross,
            place,
            *grams,
        ),
        5,
        60 * cube,
    )
    sym_two_rows = lax.dynamic_slice_in_dim(sym_two, row_start, share, 0)
    sym_one_rows = lax.dynamic_slice_in_dim(sym_one, row_start, share, 0)
    cross_rows = lax.dynamic_slice_in_dim(out_cross, row_start, share, 0)
    cross_cols = lax.dynamic_slice_in_dim(out_cross, row_start, share, 1)
    out_left_two = (
        grad_left_two
        - summed[0]
        - large(sym_two_rows, left_two, (1, 0))
        - large(cross_rows, left_one, (1, 0))
    )
    out_left_one = (
        grad_left_one
        - summed[1]
        - large(cross_cols, left_two, (0, 0))
        - large(sym_one_rows, left_one, (1, 0))
    )
    return (
        out_below,
        out_left_two,
        out_left_one,
        half_two,
        half_one,
        out_cross,
        own_two[0] if own_two else lax.dynamic_slice_in_dim(solved_two, col_start, width, 1),
        own_one[0] if own_one else lax.dynamic_slice_in_dim(solved_one, col_start, width, 1),
    )


MESH = pl.DeviceIdType.MESH


def split(values):
    high = values.astype(jnp.bfloat16)
    return high, (values - high.astype(jnp.float32)).astype(jnp.bfloat16)


def thrice(left, right, contract=(1, 0)):
    def single(one, other):
        return lax.dot_general(
            one,
            other,
            ((contract[:1], contract[1:]), ((), ())),
            preferred_element_type=jnp.float32,
        )

    return (single(left[1], right[0]) + single(left[0], right[1])) + single(left[0], right[0])


def fused_kernel(plan, *refs):
    (
        two_hbm,
        one_hbm,
        cross_hbm,
        left_two_hbm,
        left_one_hbm,
        below_hbm,
        panel_two_hbm,
        panel_one_hbm,
        grad_two_hbm,
        grad_one_hbm,
        grad_cross_hbm,
        grad_left_two_hbm,
        grad_left_one_hbm,
        grad_below_hbm,
        grad_panel_two_hbm,
        grad_panel_one_hbm,
    ) = refs[:16]
    (
        acc,
        panel_out,
        half_two,
        next_cross,
        middle_one,
        inverse_one,
        grad_left,
        left_high,
        left_low,
    ) = refs[16:25]
    (
        two,
        one,
        cross,
        left,
        below,
        panels,
        grad_two,
        grad_one,
        grad_cross,
        full_two,
        full_one,
        solved_high,
        solved_low,
        vees,
        below_high,
        below_low,
        inverse_two,
        crossed,
        pre,
        partial,
        from_core,
        chip,
        from_x,
        around,
        own,
        oth,
        lefts,
        lefts_core,
        lefts_send,
        lefts_x,
        sym_two,
        cross_t,
        load_sem,
        y_send,
        y_recv,
        z_send,
        z_recv,
        w_sent,
        w_recv,
        l_send,
        l_recv,
    ) = refs[25:]
    size = two.shape[0]
    rows, width = grad_panel_two_hbm.shape
    share = grad_left.shape[1]
    quarter = width // 2
    at_row, at_col, at_depth = (lax.axis_index(name) for name in ("row", "col", "depth"))
    core = lax.rem(at_row, 2)
    side = lax.div(at_row, 2)
    first = at_col == 0
    part = lax.rem(at_depth, 2)
    to_core = (at_row + 1 - 2 * core, at_col, at_depth)
    to_x = (at_row + 2 - 4 * side, at_col, at_depth)
    to_y = (at_row, 1 - at_col, at_depth)
    to_z = (at_row, at_col, at_depth + 1 - 2 * part)
    to_xy = (at_row + 2 - 4 * side, 1 - at_col, at_depth)

    loads = []

    def load(source, target):
        copy = pltpu.make_async_copy(source, target, load_sem.at[len(loads)])
        copy.start()
        loads.append(copy)
        return copy

    own_two = load(grad_panel_two_hbm, full_two.at[:, :width])
    pan_two = load(panel_two_hbm, panels.at[:, :width])
    pan_one = load(panel_one_hbm, panels.at[:, width:])
    own_one = load(grad_panel_one_hbm, full_one.at[:, :width])
    block_loads = [load(two_hbm, two), load(one_hbm, one)]
    small_loads = [
        load(cross_hbm, cross),
        load(grad_two_hbm, grad_two),
        load(grad_one_hbm, grad_one),
        load(grad_cross_hbm, grad_cross),
    ]
    below_load = load(below_hbm, below)
    left_loads = [load(left_two_hbm, left.at[:size]), load(left_one_hbm, left.at[size:])]
    acc_load = load(grad_below_hbm, acc)
    grad_left_loads = [
        load(grad_left_two_hbm, grad_left.at[0]),
        load(grad_left_one_hbm, grad_left.at[1]),
    ]

    barrier = pltpu.get_barrier_semaphore()
    for target in (to_core, to_x, to_y, to_z, to_xy):
        pl.semaphore_signal(barrier, inc=1, device_id=target, device_id_type=MESH)
    pl.semaphore_wait(barrier, 5)

    sends = []

    def send(source, target, sems, at, device):
        copy = pltpu.make_async_remote_copy(
            src_ref=source,
            dst_ref=target,
            send_sem=sems[0].at[at],
            recv_sem=sems[1].at[at],
            device_id=device,
            device_id_type=MESH,
        )
        copy.start()
        sends.append(copy)
        return copy

    fulls = (full_two, full_one)
    y_copies = []
    places = []
    for panel, source in enumerate((grad_panel_two_hbm, grad_panel_one_hbm)):
        forwarded, direct = plan[panel]
        extent = sum(forwarded)
        begin = 0
        for at, count in enumerate(forwarded + direct):
            if at == len(forwarded):
                begin = 2 * extent
            start = part * extent + begin if at < len(forwarded) else begin
            place = pl.ds(pl.multiple_of(start, 8), count)
            begin += count
            at = len(y_copies)
            y_copies.append(
                send(source.at[place, :], fulls[panel].at[place, width:], (y_send, y_recv), at, to_y)
            )
            places.append((panel, place))
    order = list(range(len(plan[0][0]))) + [
        len(plan[0][0]) + len(plan[0][1]) + at for at in range(len(plan[1][0]))
    ]
    z_copies = []

    def forward():
        at = order[len(z_copies)]
        y_copies[at].wait_recv()
        panel, place = places[at]
        piece = fulls[panel].at[place, width:]
        z_copies.append(send(piece, piece, (z_send, z_recv), len(z_copies), to_z))

    mine = pl.ds(pl.multiple_of(core * quarter, quarter), quarter)
    theirs = pl.ds(pl.multiple_of((1 - core) * quarter, quarter), quarter)
    waits = {}

    def w_send(name, source, target, device):
        waits[name] = send(source, target, (w_sent, w_recv), len(waits), device)

    def w_core(start, count):
        blocks = pl.ds(start, count)
        w_send(("core", start), partial.at[blocks, theirs, :], from_core.at[blocks], to_core)

    def w_chip(start, count):
        blocks = pl.ds(start, count)
        waits["core", start].wait_recv()
        chip[blocks] = partial[blocks, mine, :] + from_core[blocks]

    def w_x(start, count):
        w_chip(start, count)
        blocks = pl.ds(start, count)
        w_send(("x", start), chip.at[blocks], from_x.at[blocks], to_x)

    def w_own(start, count):
        blocks = pl.ds(start, count)
        waits["x", start].wait_recv()
        own[blocks, mine, :] = chip[blocks] + from_x[blocks]
        piece = own.at[blocks, mine, :]
        w_send(("own", start), piece, piece, to_core)

    def w_y(start, count):
        blocks = pl.ds(start, count)
        w_send(("y", start), own.at[blocks, mine, :], oth.at[blocks, mine, :], to_y)

    def w_last(start, count):
        blocks = pl.ds(start, count)
        waits["y", start].wait_recv()
        piece = oth.at[blocks, mine, :]
        w_send(("oth", start), piece, piece, to_core)

    def w_around(block):
        w_chip(block, 1)
        source = chip.at[block]
        w_send(("xy", block), source, around.at[1], to_xy)
        w_send(("y", block), source, around.at[0], to_y)
        w_send(("x", block), source, from_x.at[block], to_x)

    def w_gather(block):
        w_own(block, 1)
        waits["y", block].wait_recv()
        waits["xy", block].wait_recv()
        oth[block, mine, :] = around[0] + around[1]
        piece = oth.at[block, mine, :]
        w_send(("oth", block), piece, piece, to_core)

    def joined_at(diagonal, off):
        near, far = own[diagonal], oth[diagonal]
        near_off, far_off = own[off], oth[off]
        top = [jnp.where(first, near, far), jnp.where(first, far_off, near_off)]
        bottom = [jnp.where(first, near_off, far_off), jnp.where(first, far, near)]
        return jnp.concatenate(
            [jnp.concatenate(top, axis=1), jnp.concatenate(bottom, axis=1)], axis=0
        )

    def local_rows(values):
        near = jnp.where(first, values[:width, :], values[width:, :])
        away = jnp.where(first, values[width:, :], values[:width, :])
        return jnp.concatenate([near, away], axis=0)

    def own_columns(values):
        return jnp.where(first, values[:, :width], values[:, width:])

    def row_place(begin, count):
        return pl.ds(pl.multiple_of(begin, 8), count)

    def below_parts(place):
        return below_high[place, :], below_low[place, :]

    def off_two(place):
        return thrice(split(full_two[place, width:]), split(panels[place, :]), (0, 0))

    def off_one(place):
        return thrice(split(full_one[place, width:]), split(panels[place, width:]), (0, 0))

    def v_two(place):
        return thrice(split(full_two[place, width:]), below_parts(place), (0, 0))

    def v_one(place):
        return thrice(split(full_one[place, width:]), below_parts(place), (0, 0))

    def solve_two(place):
        total = thrice(split(full_two[place, :]), right_two)
        panel_out[0, place, :] = own_columns(total)
        high, low = split(total)
        solved_high[place, :size] = high
        solved_low[place, :size] = low

    def solve_one(place):
        both = tuple(
            jnp.concatenate([piece, before[place, :size]], axis=1)
            for piece, before in zip(split(full_one[place, :]), (solved_high, solved_low))
        )
        total = thrice(both, right_one)
        panel_out[1, place, :] = own_columns(total)
        high, low = split(total)
        solved_high[place, size:] = high
        solved_low[place, size:] = low

    l_waits = {}

    def lefts_out(panel):
        for at, away in enumerate((1 - side, side)):
            l_waits["core", panel, at] = send(
                lefts.at[panel, away, 1 - core],
                lefts_core.at[panel, at],
                (l_send, l_recv),
                panel * 3 + at,
                to_core,
            )

    def lefts_away(panel):
        l_waits["core", panel, 0].wait_recv()
        lefts_send[panel] = lefts[panel, 1 - side, core] + lefts_core[panel, 0]
        l_waits["x", panel] = send(
            lefts_send.at[panel], lefts_x.at[panel], (l_send, l_recv), panel * 3 + 2, to_x
        )

    def lefts_end(panel):
        l_waits["core", panel, 1].wait_recv()
        l_waits["x", panel].wait_recv()
        return (lefts[panel, side, core] + lefts_core[panel, 1]) + lefts_x[panel]

    tiles = 4
    tile = rows // tiles

    def below_of(panel, at):
        columns = pl.ds(panel * size, size)
        place = pl.ds(at * tile, tile)
        acc[place, :] = acc[place, :] - thrice(
            (solved_high[place, columns], solved_low[place, columns]),
            (left_high[columns, :], left_low[columns, :]),
        )

    own_two.wait()
    pan_two.wait()
    pan_one.wait()
    panel_parts = split(panels[...])
    found = thrice(split(full_two[:, :width]), panel_parts, (0, 0))
    partial[0] = found[:, :width]
    partial[1] = found[:, width:]
    own_one.wait()
    partial[2] = thrice(
        split(full_one[:, :width]), tuple(piece[:, width:] for piece in panel_parts), (0, 0)
    )
    w_core(0, 3)

    for copy in block_loads:
        copy.wait()
    grid_rows, grid_cols = grid_of(size)
    scale = jnp.where(
        grid_rows > grid_cols, 1.0, jnp.where(grid_rows == grid_cols, 0.5, 0.0)
    )
    events = {
        3: lambda: w_x(0, 3),
        4: forward,
        5: forward,
        6: forward,
    }
    mid = size // 2
    blocks = []
    for ref in (two, one):
        blocks += [ref[:mid, :mid], ref[mid:, mid:]]
    found = invert_steps(blocks, events)
    for at, (ref, inverse) in enumerate(((two, inverse_two), (one, inverse_one))):
        step_product = small(ref[mid:, :mid], found[2 * at])
        inverse[:mid, :mid] = found[2 * at]
        inverse[mid:, mid:] = found[2 * at + 1]
        inverse[:mid, mid:] = jnp.zeros((mid, size - mid), jnp.float32)
        inverse[mid:, :mid] = -small(found[2 * at + 1], step_product)
    for copy in small_loads:
        copy.wait()
    split_cross = split(cross[...])
    split_two = split(inverse_two[...])
    split_one = split(inverse_one[...])
    right_two = split(local_rows(inverse_two[...]))
    crossed_one = thrice(split_cross, split_one)
    right_one = split(jnp.concatenate([local_rows(inverse_one[...]), -crossed_one], axis=0))
    forward()
    forward()

    half = rows // 2
    near_two = row_place(part * half, half)
    far_two = row_place((1 - part) * half, half)
    extent = sum(plan[1][0])
    near_one = row_place(part * extent, extent)
    far_one = row_place((1 - part) * extent, extent)
    shared = pl.ds(2 * extent, rows - 2 * extent)
    everything = pl.ds(0, rows)

    pre[0] = thrice(split(two[...]), split(grad_two[...]), (0, 0))
    pre[1] = thrice(split(one[...]), split(grad_one[...]), (0, 0))
    forward()
    below_load.wait()
    high, low = split(below[...])
    below_high[...] = high
    below_low[...] = low
    vees[0, :width] = thrice(split(full_two[:, :width]), below_parts(everything), (0, 0))
    forward()
    vees[1, :width] = thrice(split(full_one[:, :width]), below_parts(everything), (0, 0))
    forward()
    w_own(0, 3)
    w_y(0, 2)
    off_near = off_two(near_two)
    v_near = v_two(near_two)
    solve_two(near_two)
    forward()
    crossed[...] = thrice(split_two, split_cross)
    forward()
    for copy in left_loads:
        copy.wait()
    high, low = split(left[...])
    left_high[...] = high
    left_low[...] = low
    forward()
    for at in range(len(plan[0][0])):
        z_copies[at].wait_recv()
    off = off_near + off_two(far_two)
    partial[3] = off[:, :width]
    partial[4] = off[:, width:]
    w_core(3, 2)
    forward()
    vees[0, width:] = v_near + v_two(far_two)
    solve_two(far_two)
    forward()
    found = thrice(right_two, split(vees[0]), (0, 0))
    lefts[0] = found.reshape(lefts.shape[1:])
    lefts_out(0)
    w_x(3, 2)
    while len(z_copies) < len(order):
        forward()
    off_near = off_one(near_one)
    v_near = v_one(near_one)
    vees[2] = thrice(
        tuple(piece[size:, :] for piece in right_one), split(lefts[0].reshape(size, -1)), (0, 0)
    )
    lefts_away(0)
    solve_one(near_one)
    acc_load.wait()
    for at in range(tiles):
        below_of(0, at)
    w_own(3, 2)
    w_y(3, 2)
    for at in range(len(plan[0][0]), len(order)):
        z_copies[at].wait_recv()
    off = off_near + off_one(far_one)
    v_far = v_near + v_one(far_one)
    for at in range(len(plan[1][1])):
        y_copies[len(y_copies) - 1 - at].wait_recv()
    partial[5] = off + off_one(shared)
    w_core(5, 1)
    vees[1, width:] = v_far + v_one(shared)
    found = vees[2] + thrice(
        tuple(piece[:size, :] for piece in right_one), split(vees[1]), (0, 0)
    )
    lefts[1] = found.reshape(lefts.shape[1:])
    lefts_out(1)
    w_last(0, 2)
    w_around(5)
    solve_one(far_one)
    solve_one(shared)
    lefts_away(1)
    w_y(2, 1)
    below_of(1, 0)
    below_of(1, 1)
    w_last(3, 2)
    below_of(1, 2)
    below_of(1, 3)
    for start in (0, 3):
        waits["own", start].wait_recv()
        waits["oth", start].wait_recv()

    inner = scale * (pre[0] - joined_at(0, 3))
    middle = split(inner + inner.T)
    cross_gram = thrice(split_two, split(joined_at(1, 4)), (0, 0))
    spread = thrice(
        split_two,
        split(
            thrice(
                middle, split(jnp.concatenate([inverse_two[...], crossed[...]], axis=1))
            )
        ),
        (0, 0),
    )
    sym_two[...] = spread[:, :size]
    half_two[...] = scale * spread[:, :size]
    following = split(grad_cross[...] - cross_gram - spread[:, size:])
    found = thrice(following, split_one)
    next_cross[...] = found
    cross_t[...] = found.T
    ready = pre[1] - (
        thrice(following, split_cross, (0, 0)) - thrice(split_cross, split(cross_gram), (0, 0))
    )
    w_gather(5)
    w_last(2, 1)
    mine_rows = pl.ds(pl.multiple_of(at_row * share, share), share)
    for copy in grad_left_loads:
        copy.wait()
    head = split(jnp.concatenate([sym_two[mine_rows, :], next_cross[mine_rows, :]], axis=1))
    grad_left[0] = (grad_left[0] - lefts_end(0)) - thrice(
        head, (left_high[...], left_low[...])
    )
    last = grad_left[1] - thrice(split(cross_t[mine_rows, :]), (left_high[:size], left_low[:size]))
    grad_left[1] = last - lefts_end(1)
    for start in (2, 5):
        waits["oth", start].wait_recv()
    waits["own", 5].wait_recv()
    inner = scale * (ready - joined_at(2, 5))
    middle_one[...] = inner + inner.T
    for copy in sends:
        copy.wait_send()


def tail_kernel(*refs):
    (
        acc,
        panel_out,
        half_two,
        next_cross,
        middle_one,
        inverse_one,
        grad_left,
        left_high,
        left_low,
    ) = refs[:9]
    (
        out_below,
        out_left_two,
        out_left_one,
        out_diag_two,
        out_diag_one,
        out_cross,
        out_panel_two,
        out_panel_one,
    ) = refs[9:17]
    sym_one, half_one, last, store_sem = refs[17:]
    size = sym_one.shape[0]
    share = last.shape[0]
    stores = []

    def store(source, target):
        copy = pltpu.make_async_copy(source, target, store_sem.at[len(stores)])
        copy.start()
        stores.append(copy)

    store(acc, out_below)
    store(panel_out.at[0], out_panel_two)
    store(panel_out.at[1], out_panel_one)
    store(half_two, out_diag_two)
    store(next_cross, out_cross)
    store(grad_left.at[0], out_left_two)
    inverse = split(inverse_one[...])
    found = thrice(inverse, split(thrice(split(middle_one[...]), inverse)), (0, 0))
    sym_one[...] = found
    rows, cols = grid_of(size)
    half_one[...] = jnp.where(rows > cols, found, jnp.where(rows == cols, 0.5 * found, 0.0))
    store(half_one, out_diag_one)
    mine_rows = pl.ds(pl.multiple_of(lax.axis_index("row") * share, share), share)
    last[...] = grad_left[1] - thrice(
        split(sym_one[mine_rows, :]), (left_high[size:, :], left_low[size:, :])
    )
    store(last, out_left_one)
    for copy in stores:
        copy.wait()


def invert_steps(blocks, events):
    size = blocks[0].shape[0]
    rows, cols = grid_of(size)
    apart = rows ^ cols
    lower = rows > cols
    inverses = []
    for block in blocks:
        diagonal = jnp.where(rows == cols, block, 0.0)
        down = 1.0 / jnp.sum(diagonal, axis=1, keepdims=True)
        across = 1.0 / jnp.sum(diagonal, axis=0, keepdims=True)
        pair = jnp.where(lower & (apart == 1), block, 0.0)
        inverses.append(jnp.where(rows == cols, down, 0.0) - pair * down * across)
    level = 1
    while (2 << level) <= size:
        mask = lower & ((apart >> level) == 1)
        steps = [
            small(jnp.where(mask, block, 0.0), inverse) for block, inverse in zip(blocks, inverses)
        ]
        inverses = [inverse - small(inverse, step) for inverse, step in zip(inverses, steps)]
        if level in events:
            events[level]()
        level += 1
    for late in sorted(events):
        if late >= level:
            events[late]()
    return inverses


def fused(*arrays):
    two, left, below, grad_left = arrays[0], arrays[3], arrays[5], arrays[11]
    size = two.shape[0]
    rows, width = arrays[14].shape
    columns = below.shape[1]
    share = grad_left.shape[0]
    quarter = width // 2
    piece = rows // 8
    plan = (
        ([piece // 2] * 8, []),
        ([piece // 2] * 6, [piece] * 2),
    )
    y_count = sum(len(go) + len(stay) for go, stay in plan)
    z_count = sum(len(go) for go, _ in plan)

    def real(*shape):
        return pltpu.VMEM(shape, jnp.float32)

    def short(*shape):
        return pltpu.VMEM(shape, jnp.bfloat16)

    def outs(*shape):
        return jax.ShapeDtypeStruct(shape, jnp.float32)

    scratch = [
        real(size, size),
        real(size, size),
        real(size, size),
        real(2 * size, columns),
        real(rows, columns),
        real(rows, size),
        real(size, size),
        real(size, size),
        real(size, size),
        real(rows, size),
        real(rows, size),
        short(rows, 2 * size),
        short(rows, 2 * size),
        real(3, size, columns),
        short(rows, columns),
        short(rows, columns),
        real(size, size),
        real(size, size),
        real(2, size, size),
        real(6, width, width),
        real(6, quarter, width),
        real(6, quarter, width),
        real(6, quarter, width),
        real(2, quarter, width),
        real(6, width, width),
        real(6, width, width),
        real(2, 2, 2, share, columns),
        real(2, 2, share, columns),
        real(2, share, columns),
        real(2, share, columns),
        real(size, size),
        real(size, size),
        pltpu.SemaphoreType.DMA((16,)),
        pltpu.SemaphoreType.DMA((y_count,)),
        pltpu.SemaphoreType.DMA((y_count,)),
        pltpu.SemaphoreType.DMA((z_count,)),
        pltpu.SemaphoreType.DMA((z_count,)),
        pltpu.SemaphoreType.DMA((18,)),
        pltpu.SemaphoreType.DMA((18,)),
        pltpu.SemaphoreType.DMA((6,)),
        pltpu.SemaphoreType.DMA((6,)),
    ]
    anywhere = pl.BlockSpec(memory_space=pl.ANY)
    near = pl.BlockSpec(memory_space=pltpu.VMEM)
    far = pl.BlockSpec(memory_space=pltpu.HBM)
    kept = pl.pallas_call(
        lambda *refs: fused_kernel(plan, *refs),
        out_shape=[
            real(rows, columns),
            real(2, rows, width),
            real(size, size),
            real(size, size),
            real(size, size),
            real(size, size),
            real(2, share, columns),
            short(2 * size, columns),
            short(2 * size, columns),
        ],
        in_specs=[far] * 16,
        out_specs=[near] * 9,
        scratch_shapes=scratch,
        compiler_params=pltpu.CompilerParams(
            collective_id=0,
            has_side_effects=True,
            vmem_limit_bytes=40 << 20,
        ),
        cost_estimate=pl.CostEstimate(
            flops=24 * rows * size * columns, bytes_accessed=16 * rows * columns, transcendentals=0
        ),
    )(*[pltpu.with_memory_space_constraint(values, pltpu.HBM) for values in arrays])
    return pl.pallas_call(
        tail_kernel,
        out_shape=[
            outs(rows, columns),
            outs(share, columns),
            outs(share, columns),
            outs(size, size),
            outs(size, size),
            outs(size, size),
            outs(rows, width),
            outs(rows, width),
        ],
        in_specs=[near] * 9,
        out_specs=[anywhere] * 8,
        scratch_shapes=[
            real(size, size),
            real(size, size),
            real(share, columns),
            pltpu.SemaphoreType.DMA((8,)),
        ],
        compiler_params=pltpu.CompilerParams(vmem_limit_bytes=8 << 20),
        cost_estimate=pl.CostEstimate(
            flops=12 * size**3, bytes_accessed=8 * rows * columns, transcendentals=0
        ),
    )(*[pltpu.with_memory_space_constraint(values, pltpu.VMEM) for values in kept])


def fits(mesh):
    return mesh.shape["row"] == 4 and mesh.shape["col"] == 2 and mesh.shape["depth"] % 2 == 0


def solution(mesh):
    panels = P("row", "col")
    lefts = P(None, ("col", "depth"))
    blocks = P("row", ("col", "depth"))
    return jax.shard_map(
        fused if fits(mesh) else body,
        mesh=mesh,
        in_specs=(P(), P(), P(), lefts, lefts, blocks, panels, panels)
        + (P(), P(), P(), blocks, blocks, blocks, panels, panels),
        out_specs=(blocks, blocks, blocks, P(), P(), P(), panels, panels),
        check_vma=False,
    )
```

```python
import jax
import jax.numpy as jnp
from jax import lax
from jax.experimental import pallas as pl
from jax.experimental.pallas import tpu as pltpu
from jax.sharding import PartitionSpec as P


def large(left, right, contract):
    return lax.dot_general(
        left,
        right,
        ((contract[:1], contract[1:]), ((), ())),
        precision=lax.Precision.HIGH,
        preferred_element_type=jnp.float32,
    )


def small(left, right, contract=(1, 0)):
    return lax.dot_general(
        left,
        right,
        ((contract[:1], contract[1:]), ((), ())),
        precision=lax.Precision.HIGHEST,
        preferred_element_type=jnp.float32,
    )


def grid_of(size):
    rows = lax.broadcasted_iota(jnp.int32, (size, size), 0)
    cols = lax.broadcasted_iota(jnp.int32, (size, size), 1)
    return rows, cols


def invert_all(blocks):
    size = blocks[0].shape[0]
    rows, cols = grid_of(size)
    apart = rows ^ cols
    lower = rows > cols
    inverses = []
    for block in blocks:
        diagonal = jnp.where(rows == cols, block, 0.0)
        down = 1.0 / jnp.sum(diagonal, axis=1, keepdims=True)
        across = 1.0 / jnp.sum(diagonal, axis=0, keepdims=True)
        pair = jnp.where(lower & (apart == 1), block, 0.0)
        inverses.append(jnp.where(rows == cols, down, 0.0) - pair * down * across)
    level = 1
    while (2 << level) <= size:
        mask = lower & ((apart >> level) == 1)
        steps = [
            small(jnp.where(mask, block, 0.0), inverse) for block, inverse in zip(blocks, inverses)
        ]
        inverses = [inverse - small(inverse, step) for inverse, step in zip(inverses, steps)]
        level += 1
    return inverses


def invert_kernel(two_ref, one_ref, cross_ref, inv_two_ref, inv_one_ref, cross_inv_ref):
    half = two_ref.shape[0] // 2
    refs = (two_ref, one_ref)
    outs = (inv_two_ref, inv_one_ref)
    blocks = []
    for ref in refs:
        blocks += [ref[:half, :half], ref[half:, half:]]
    inverses = invert_all(blocks)
    steps = [small(ref[half:, :half], inverses[2 * at]) for at, ref in enumerate(refs)]
    for at, out in enumerate(outs):
        out[:half, :half] = inverses[2 * at]
        out[half:, half:] = inverses[2 * at + 1]
        out[:half, half:] = jnp.zeros((half, half), jnp.float32)
        out[half:, :half] = -small(inverses[2 * at + 1], steps[at])
    cross_inv_ref[...] = small(cross_ref[...], inv_one_ref[...])


def chain_kernel(
    two_ref,
    one_ref,
    cross_ref,
    inv_two_ref,
    inv_one_ref,
    grad_two_ref,
    grad_one_ref,
    grad_cross_ref,
    place_ref,
    *rest,
):
    grams, outs = rest[:-5], rest[-5:]
    chain(
        two_ref,
        one_ref,
        cross_ref,
        inv_two_ref,
        inv_one_ref,
        grad_two_ref,
        grad_one_ref,
        grad_cross_ref,
        joined(grams, place_ref),
        *outs,
    )


def joined(grams, place_ref):
    if len(grams) == 1:
        return grams[0][...]
    mine, beside, twin, across = [gram[...] for gram in grams]
    left = place_ref[0] == 0
    upper = place_ref[1] == 0
    own = jnp.concatenate([jnp.where(left, mine, beside), jnp.where(left, beside, mine)], axis=1)
    far = jnp.concatenate([jnp.where(left, twin, across), jnp.where(left, across, twin)], axis=1)
    return jnp.concatenate([jnp.where(upper, own, far), jnp.where(upper, far, own)], axis=0)


def chain(
    two_ref,
    one_ref,
    cross_ref,
    inv_two_ref,
    inv_one_ref,
    grad_two_ref,
    grad_one_ref,
    grad_cross_ref,
    grams,
    sym_two_ref,
    sym_one_ref,
    half_two_ref,
    half_one_ref,
    out_cross_ref,
):
    size = two_ref.shape[0]
    rows, cols = grid_of(size)
    lower = rows >= cols
    scale = jnp.where(rows > cols, 1.0, jnp.where(rows == cols, 0.5, 0.0))

    def sym(factor, inverse, cotangent):
        inner = scale * small(factor, cotangent, (0, 0))
        spread = small(small(inverse, inner, (0, 0)), inverse)
        return spread + spread.T

    gram_two = grams[:size, :]
    gram_cross = grams[size : 2 * size, :]
    gram_below = grams[2 * size :, :]
    sym_two = sym(
        two_ref[...], inv_two_ref[...], grad_two_ref[...] - jnp.where(lower, gram_two, 0.0)
    )
    sym_two_ref[...] = sym_two
    half_two_ref[...] = scale * sym_two
    cross_next = grad_cross_ref[...] - gram_cross - small(sym_two, cross_ref[...])
    out_cross = small(cross_next, inv_one_ref[...])
    out_cross_ref[...] = out_cross
    gram_one = small(out_cross, cross_ref[...], (0, 0)) + gram_below
    sym_one = sym(
        one_ref[...], inv_one_ref[...], grad_one_ref[...] - jnp.where(lower, gram_one, 0.0)
    )
    sym_one_ref[...] = sym_one
    half_one_ref[...] = scale * sym_one


def local_call(kernel, operands, count, flops):
    size = operands[0].shape[0]
    moved = 4 * size * size * (len(operands) + count)
    return pl.pallas_call(
        kernel,
        out_shape=[jax.ShapeDtypeStruct((size, size), jnp.float32)] * count,
        in_specs=[
            pl.BlockSpec(memory_space=pltpu.SMEM if operand.ndim == 1 else pltpu.VMEM)
            for operand in operands
        ],
        out_specs=[pl.BlockSpec(memory_space=pltpu.VMEM)] * count,
        cost_estimate=pl.CostEstimate(flops=flops, bytes_accessed=moved, transcendentals=0),
    )(*operands)


def swap(values, axis, bit):
    size = lax.axis_size(axis)
    return lax.ppermute(values, axis, [(at, at ^ bit) for at in range(size)])


def gathered(values, axis):
    if lax.axis_size(axis) != 2:
        return [(lax.all_gather(values, axis, axis=1, tiled=True), 0)]
    width = values.shape[1]
    at = lax.axis_index(axis)
    return [(values, at * width), (swap(values, axis, 1), (1 - at) * width)]


def parted(values):
    high = values.astype(jnp.bfloat16)
    return high, (values - high.astype(jnp.float32)).astype(jnp.bfloat16)


def product(left, right):
    (left_high, left_low), (right_high, right_low) = parted(left), parted(right)

    def single(one, other):
        return jnp.dot(one, other, preferred_element_type=jnp.float32)

    return (single(left_low, right_high) + single(left_high, right_low)) + single(
        left_high, right_high
    )


def solve_kernel(count, starts_ref, inverse_ref, *refs):
    pieces, extra, outs = refs[:count], refs[count:-count], refs[-count:]
    total = None
    for at, piece in enumerate(pieces):
        width = piece.shape[1]
        rows = inverse_ref[pl.ds(pl.multiple_of(starts_ref[at], width), width), :]
        part = product(piece[...], rows)
        total = part if total is None else total + part
    if extra:
        total = total - product(extra[0][...], extra[1][...])
    outs[0][...] = total
    if count > 1:
        width = outs[1].shape[1]
        outs[1][...] = jnp.where(starts_ref[0] == 0, total[:, :width], total[:, width:])


def solve(pieces, inverse, *extra):
    count = len(pieces)
    rows, width = pieces[0][0].shape
    size = inverse.shape[0]
    block = rows // 4
    starts = jnp.stack([jnp.asarray(start, jnp.int32) for _, start in pieces])

    def tall(columns):
        return pl.BlockSpec((block, columns), lambda step: (step, 0))

    whole = pl.BlockSpec((size, size), lambda step: (0, 0))
    widths = [size, width][:count]
    return pl.pallas_call(
        lambda *refs: solve_kernel(count, *refs),
        grid=(4,),
        out_shape=[jax.ShapeDtypeStruct((rows, columns), jnp.float32) for columns in widths],
        in_specs=[pl.BlockSpec(memory_space=pltpu.SMEM), whole]
        + [tall(values.shape[1]) for values, _ in pieces]
        + ([tall(size), whole] if extra else []),
        out_specs=[tall(columns) for columns in widths],
        cost_estimate=pl.CostEstimate(
            flops=6 * rows * size * size, bytes_accessed=12 * rows * size, transcendentals=0
        ),
    )(starts, inverse, *[values for values, _ in pieces], *extra)


def assembled(values, axis):
    size = lax.axis_size(axis)
    if size != 2:
        return lax.all_gather(values, axis, axis=1, tiled=True)
    other = swap(values, axis, 1)
    first = lax.axis_index(axis) == 0
    return jnp.concatenate(
        [jnp.where(first, values, other), jnp.where(first, other, values)], axis=1
    )


def halve(values, axis, bit):
    mine = (lax.axis_index(axis) // bit) % 2
    keep = lax.dynamic_index_in_dim(values, mine, 0, keepdims=False)
    give = lax.dynamic_index_in_dim(values, 1 - mine, 0, keepdims=False)
    return keep + swap(give, axis, bit)


def scatter_sum(values, axis):
    size = lax.axis_size(axis)
    if size & (size - 1):
        return lax.psum_scatter(values, axis, scatter_dimension=0, tiled=False)
    bit = 1
    while bit < size:
        paired = values.reshape((-1, 2) + values.shape[1:])
        values = halve(jnp.moveaxis(paired, 1, 0), axis, bit)
        bit *= 2
    return values[0]


def row_sum(values, axis, columns):
    size = lax.axis_size(axis)
    if size & (size - 1) or size < 2:
        return [assembled(lax.psum(values, axis), columns)]
    part = halve(values.reshape((2, -1) + values.shape[1:]), axis, 1)
    bit = 2
    while bit < size:
        part = part + swap(part, axis, bit)
        bit *= 2
    if lax.axis_size(columns) == 2:
        beside = swap(part, columns, 1)
        return [part, beside, swap(part, axis, 1), swap(beside, axis, 1)]
    part = assembled(part, columns)
    other = swap(part, axis, 1)
    even = lax.axis_index(axis) % 2 == 0
    return [jnp.concatenate([jnp.where(even, part, other), jnp.where(even, other, part)], axis=0)]


def body(
    diag_two,
    diag_one,
    cross_tile,
    left_two,
    left_one,
    below_left,
    panel_two,
    panel_one,
    grad_diag_two,
    grad_diag_one,
    grad_cross,
    grad_left_two,
    grad_left_one,
    grad_below,
    grad_panel_two,
    grad_panel_one,
):
    size = diag_two.shape[0]
    share = grad_left_two.shape[0]
    width = panel_two.shape[1]
    row_start = lax.axis_index("row") * share
    col_start = lax.axis_index("col") * width
    cube = 2 * size**3

    pieces_two = gathered(grad_panel_two, "col")
    pieces_one = gathered(grad_panel_one, "col")
    inv_two, inv_one, cross_inv = local_call(
        invert_kernel, (diag_two, diag_one, cross_tile), 3, 60 * cube
    )
    solved_two, *own_two = solve(pieces_two, inv_two)
    solved_one, *own_one = solve(pieces_one, inv_one, solved_two, cross_inv)
    place = jnp.stack([lax.axis_index("col"), lax.axis_index("row") % 2]).astype(jnp.int32)
    partial = jnp.concatenate(
        [
            large(solved_two, panel_two, (0, 0)),
            large(solved_two, panel_one, (0, 0)),
            large(solved_one, panel_one, (0, 0)),
        ],
        axis=0,
    )
    grams = row_sum(partial, "row", "col")
    rows = lax.axis_size("row")
    lefts = jnp.stack(
        [
            large(solved_two, below_left, (0, 0)).reshape(rows, share, -1),
            large(solved_one, below_left, (0, 0)).reshape(rows, share, -1),
        ],
        axis=1,
    )
    summed = scatter_sum(lefts, "row")
    out_below = (
        grad_below - large(solved_two, left_two, (1, 0)) - large(solved_one, left_one, (1, 0))
    )
    sym_two, sym_one, half_two, half_one, out_cross = local_call(
        chain_kernel,
        (
            diag_two,
            diag_one,
            cross_tile,
            inv_two,
            inv_one,
            grad_diag_two,
            grad_diag_one,
            grad_cross,
            place,
            *grams,
        ),
        5,
        60 * cube,
    )
    sym_two_rows = lax.dynamic_slice_in_dim(sym_two, row_start, share, 0)
    sym_one_rows = lax.dynamic_slice_in_dim(sym_one, row_start, share, 0)
    cross_rows = lax.dynamic_slice_in_dim(out_cross, row_start, share, 0)
    cross_cols = lax.dynamic_slice_in_dim(out_cross, row_start, share, 1)
    out_left_two = (
        grad_left_two
        - summed[0]
        - large(sym_two_rows, left_two, (1, 0))
        - large(cross_rows, left_one, (1, 0))
    )
    out_left_one = (
        grad_left_one
        - summed[1]
        - large(cross_cols, left_two, (0, 0))
        - large(sym_one_rows, left_one, (1, 0))
    )
    return (
        out_below,
        out_left_two,
        out_left_one,
        half_two,
        half_one,
        out_cross,
        own_two[0] if own_two else lax.dynamic_slice_in_dim(solved_two, col_start, width, 1),
        own_one[0] if own_one else lax.dynamic_slice_in_dim(solved_one, col_start, width, 1),
    )


MESH = pl.DeviceIdType.MESH


def split(values):
    high = values.astype(jnp.bfloat16)
    return high, (values - high.astype(jnp.float32)).astype(jnp.bfloat16)


def thrice(left, right, contract=(1, 0)):
    def single(one, other):
        return lax.dot_general(
            one,
            other,
            ((contract[:1], contract[1:]), ((), ())),
            preferred_element_type=jnp.float32,
        )

    return (single(left[1], right[0]) + single(left[0], right[1])) + single(left[0], right[0])


def fused_kernel(plan, *refs):
    (
        two_hbm,
        one_hbm,
        cross_hbm,
        left_two_hbm,
        left_one_hbm,
        below_hbm,
        panel_two_hbm,
        panel_one_hbm,
        grad_two_hbm,
        grad_one_hbm,
        grad_cross_hbm,
        grad_left_two_hbm,
        grad_left_one_hbm,
        grad_below_hbm,
        grad_panel_two_hbm,
        grad_panel_one_hbm,
    ) = refs[:16]
    (
        acc,
        panel_out,
        half_two,
        next_cross,
        middle_one,
        inverse_one,
        grad_left,
        left_high,
        left_low,
    ) = refs[16:25]
    (
        two,
        one,
        cross,
        left,
        below,
        panels,
        grad_two,
        grad_one,
        grad_cross,
        full_two,
        full_one,
        solved_high,
        solved_low,
        vees,
        below_high,
        below_low,
        inverse_two,
        crossed,
        pre,
        partial,
        from_core,
        chip,
        from_x,
        around,
        own,
        oth,
        lefts,
        lefts_core,
        lefts_send,
        lefts_x,
        sym_two,
        cross_t,
        load_sem,
        y_send,
        y_recv,
        z_send,
        z_recv,
        w_sent,
        w_recv,
        l_send,
        l_recv,
    ) = refs[25:]
    size = two.shape[0]
    rows, width = grad_panel_two_hbm.shape
    share = grad_left.shape[1]
    quarter = width // 2
    at_row, at_col, at_depth = (lax.axis_index(name) for name in ("row", "col", "depth"))
    core = lax.rem(at_row, 2)
    side = lax.div(at_row, 2)
    first = at_col == 0
    part = lax.rem(at_depth, 2)
    to_core = (at_row + 1 - 2 * core, at_col, at_depth)
    to_x = (at_row + 2 - 4 * side, at_col, at_depth)
    to_y = (at_row, 1 - at_col, at_depth)
    to_z = (at_row, at_col, at_depth + 1 - 2 * part)
    to_xy = (at_row + 2 - 4 * side, 1 - at_col, at_depth)

    loads = []

    def load(source, target):
        copy = pltpu.make_async_copy(source, target, load_sem.at[len(loads)])
        copy.start()
        loads.append(copy)
        return copy

    own_two = load(grad_panel_two_hbm, full_two.at[:, :width])
    pan_two = load(panel_two_hbm, panels.at[:, :width])
    pan_one = load(panel_one_hbm, panels.at[:, width:])
    own_one = load(grad_panel_one_hbm, full_one.at[:, :width])
    block_loads = [load(two_hbm, two), load(one_hbm, one)]
    small_loads = [
        load(cross_hbm, cross),
        load(grad_two_hbm, grad_two),
        load(grad_one_hbm, grad_one),
        load(grad_cross_hbm, grad_cross),
    ]
    below_load = load(below_hbm, below)
    left_loads = [load(left_two_hbm, left.at[:size]), load(left_one_hbm, left.at[size:])]
    acc_load = load(grad_below_hbm, acc)
    grad_left_loads = [
        load(grad_left_two_hbm, grad_left.at[0]),
        load(grad_left_one_hbm, grad_left.at[1]),
    ]

    barrier = pltpu.get_barrier_semaphore()
    for target in (to_core, to_x, to_y, to_z, to_xy):
        pl.semaphore_signal(barrier, inc=1, device_id=target, device_id_type=MESH)
    pl.semaphore_wait(barrier, 5)

    sends = []

    def send(source, target, sems, at, device):
        copy = pltpu.make_async_remote_copy(
            src_ref=source,
            dst_ref=target,
            send_sem=sems[0].at[at],
            recv_sem=sems[1].at[at],
            device_id=device,
            device_id_type=MESH,
        )
        copy.start()
        sends.append(copy)
        return copy

    fulls = (full_two, full_one)
    y_copies = []
    places = []
    for panel, source in enumerate((grad_panel_two_hbm, grad_panel_one_hbm)):
        forwarded, direct = plan[panel]
        extent = sum(forwarded)
        begin = 0
        for at, count in enumerate(forwarded + direct):
            if at == len(forwarded):
                begin = 2 * extent
            start = part * extent + begin if at < len(forwarded) else begin
            place = pl.ds(pl.multiple_of(start, 8), count)
            begin += count
            at = len(y_copies)
            y_copies.append(
                send(source.at[place, :], fulls[panel].at[place, width:], (y_send, y_recv), at, to_y)
            )
            places.append((panel, place))
    order = list(range(len(plan[0][0]))) + [
        len(plan[0][0]) + len(plan[0][1]) + at for at in range(len(plan[1][0]))
    ]
    z_copies = []

    def forward():
        at = order[len(z_copies)]
        y_copies[at].wait_recv()
        panel, place = places[at]
        piece = fulls[panel].at[place, width:]
        z_copies.append(send(piece, piece, (z_send, z_recv), len(z_copies), to_z))

    mine = pl.ds(pl.multiple_of(core * quarter, quarter), quarter)
    theirs = pl.ds(pl.multiple_of((1 - core) * quarter, quarter), quarter)
    waits = {}

    def w_send(name, source, target, device):
        waits[name] = send(source, target, (w_sent, w_recv), len(waits), device)

    def w_core(start, count):
        blocks = pl.ds(start, count)
        w_send(("core", start), partial.at[blocks, theirs, :], from_core.at[blocks], to_core)

    def w_chip(start, count):
        blocks = pl.ds(start, count)
        waits["core", start].wait_recv()
        chip[blocks] = partial[blocks, mine, :] + from_core[blocks]

    def w_x(start, count):
        w_chip(start, count)
        blocks = pl.ds(start, count)
        w_send(("x", start), chip.at[blocks], from_x.at[blocks], to_x)

    def w_own(start, count):
        blocks = pl.ds(start, count)
        waits["x", start].wait_recv()
        own[blocks, mine, :] = chip[blocks] + from_x[blocks]
        piece = own.at[blocks, mine, :]
        w_send(("own", start), piece, piece, to_core)

    def w_y(start, count):
        blocks = pl.ds(start, count)
        w_send(("y", start), own.at[blocks, mine, :], oth.at[blocks, mine, :], to_y)

    def w_last(start, count):
        blocks = pl.ds(start, count)
        waits["y", start].wait_recv()
        piece = oth.at[blocks, mine, :]
        w_send(("oth", start), piece, piece, to_core)

    def w_around(block):
        w_chip(block, 1)
        source = chip.at[block]
        w_send(("xy", block), source, around.at[1], to_xy)
        w_send(("y", block), source, around.at[0], to_y)
        w_send(("x", block), source, from_x.at[block], to_x)

    def w_gather(block):
        w_own(block, 1)
        waits["y", block].wait_recv()
        waits["xy", block].wait_recv()
        oth[block, mine, :] = around[0] + around[1]
        piece = oth.at[block, mine, :]
        w_send(("oth", block), piece, piece, to_core)

    def joined_at(diagonal, off):
        near, far = own[diagonal], oth[diagonal]
        near_off, far_off = own[off], oth[off]
        top = [jnp.where(first, near, far), jnp.where(first, far_off, near_off)]
        bottom = [jnp.where(first, near_off, far_off), jnp.where(first, far, near)]
        return jnp.concatenate(
            [jnp.concatenate(top, axis=1), jnp.concatenate(bottom, axis=1)], axis=0
        )

    def local_rows(values):
        near = jnp.where(first, values[:width, :], values[width:, :])
        away = jnp.where(first, values[width:, :], values[:width, :])
        return jnp.concatenate([near, away], axis=0)

    def own_columns(values):
        return jnp.where(first, values[:, :width], values[:, width:])

    def row_place(begin, count):
        return pl.ds(pl.multiple_of(begin, 8), count)

    def below_parts(place):
        return below_high[place, :], below_low[place, :]

    def off_two(place):
        return thrice(split(full_two[place, width:]), split(panels[place, :]), (0, 0))

    def off_one(place):
        return thrice(split(full_one[place, width:]), split(panels[place, width:]), (0, 0))

    def v_two(place):
        return thrice(split(full_two[place, width:]), below_parts(place), (0, 0))

    def v_one(place):
        return thrice(split(full_one[place, width:]), below_parts(place), (0, 0))

    def solve_two(place):
        total = thrice(split(full_two[place, :]), right_two)
        panel_out[0, place, :] = own_columns(total)
        high, low = split(total)
        solved_high[place, :size] = high
        solved_low[place, :size] = low

    def solve_one(place):
        both = tuple(
            jnp.concatenate([piece, before[place, :size]], axis=1)
            for piece, before in zip(split(full_one[place, :]), (solved_high, solved_low))
        )
        total = thrice(both, right_one)
        panel_out[1, place, :] = own_columns(total)
        high, low = split(total)
        solved_high[place, size:] = high
        solved_low[place, size:] = low

    l_waits = {}

    def lefts_out(panel):
        for at, away in enumerate((1 - side, side)):
            l_waits["core", panel, at] = send(
                lefts.at[panel, away, 1 - core],
                lefts_core.at[panel, at],
                (l_send, l_recv),
                panel * 3 + at,
                to_core,
            )

    def lefts_away(panel):
        l_waits["core", panel, 0].wait_recv()
        lefts_send[panel] = lefts[panel, 1 - side, core] + lefts_core[panel, 0]
        l_waits["x", panel] = send(
            lefts_send.at[panel], lefts_x.at[panel], (l_send, l_recv), panel * 3 + 2, to_x
        )

    def lefts_end(panel):
        l_waits["core", panel, 1].wait_recv()
        l_waits["x", panel].wait_recv()
        return (lefts[panel, side, core] + lefts_core[panel, 1]) + lefts_x[panel]

    tiles = 4
    tile = rows // tiles

    def below_of(panel, at):
        columns = pl.ds(panel * size, size)
        place = pl.ds(at * tile, tile)
        acc[place, :] = acc[place, :] - thrice(
            (solved_high[place, columns], solved_low[place, columns]),
            (left_high[columns, :], left_low[columns, :]),
        )

    own_two.wait()
    pan_two.wait()
    pan_one.wait()
    panel_parts = split(panels[...])
    found = thrice(split(full_two[:, :width]), panel_parts, (0, 0))
    partial[0] = found[:, :width]
    partial[1] = found[:, width:]
    own_one.wait()
    partial[2] = thrice(
        split(full_one[:, :width]), tuple(piece[:, width:] for piece in panel_parts), (0, 0)
    )
    w_core(0, 3)

    for copy in block_loads:
        copy.wait()
    grid_rows, grid_cols = grid_of(size)
    scale = jnp.where(
        grid_rows > grid_cols, 1.0, jnp.where(grid_rows == grid_cols, 0.5, 0.0)
    )
    events = {
        3: lambda: w_x(0, 3),
        4: forward,
        5: forward,
        6: forward,
    }
    mid = size // 2
    blocks = []
    for ref in (two, one):
        blocks += [ref[:mid, :mid], ref[mid:, mid:]]
    found = invert_steps(blocks, events)
    for at, (ref, inverse) in enumerate(((two, inverse_two), (one, inverse_one))):
        step_product = small(ref[mid:, :mid], found[2 * at])
        inverse[:mid, :mid] = found[2 * at]
        inverse[mid:, mid:] = found[2 * at + 1]
        inverse[:mid, mid:] = jnp.zeros((mid, size - mid), jnp.float32)
        inverse[mid:, :mid] = -small(found[2 * at + 1], step_product)
    for copy in small_loads:
        copy.wait()
    split_cross = split(cross[...])
    split_two = split(inverse_two[...])
    split_one = split(inverse_one[...])
    right_two = split(local_rows(inverse_two[...]))
    crossed_one = thrice(split_cross, split_one)
    right_one = split(jnp.concatenate([local_rows(inverse_one[...]), -crossed_one], axis=0))
    forward()
    forward()

    half = rows // 2
    near_two = row_place(part * half, half)
    far_two = row_place((1 - part) * half, half)
    extent = sum(plan[1][0])
    near_one = row_place(part * extent, extent)
    far_one = row_place((1 - part) * extent, extent)
    shared = pl.ds(2 * extent, rows - 2 * extent)
    everything = pl.ds(0, rows)

    pre[0] = thrice(split(two[...]), split(grad_two[...]), (0, 0))
    pre[1] = thrice(split(one[...]), split(grad_one[...]), (0, 0))
    forward()
    below_load.wait()
    high, low = split(below[...])
    below_high[...] = high
    below_low[...] = low
    vees[0, :width] = thrice(split(full_two[:, :width]), below_parts(everything), (0, 0))
    forward()
    vees[1, :width] = thrice(split(full_one[:, :width]), below_parts(everything), (0, 0))
    forward()
    w_own(0, 3)
    w_y(0, 2)
    off_near = off_two(near_two)
    v_near = v_two(near_two)
    solve_two(near_two)
    forward()
    crossed[...] = thrice(split_two, split_cross)
    forward()
    for copy in left_loads:
        copy.wait()
    high, low = split(left[...])
    left_high[...] = high
    left_low[...] = low
    forward()
    for at in range(len(plan[0][0])):
        z_copies[at].wait_recv()
    off = off_near + off_two(far_two)
    partial[3] = off[:, :width]
    partial[4] = off[:, width:]
    w_core(3, 2)
    forward()
    vees[0, width:] = v_near + v_two(far_two)
    solve_two(far_two)
    forward()
    w_x(3, 2)
    found = thrice(right_two, split(vees[0]), (0, 0))
    lefts[0] = found.reshape(lefts.shape[1:])
    lefts_out(0)
    while len(z_copies) < len(order):
        forward()
    off_near = off_one(near_one)
    v_near = v_one(near_one)
    vees[2] = thrice(
        tuple(piece[size:, :] for piece in right_one), split(lefts[0].reshape(size, -1)), (0, 0)
    )
    lefts_away(0)
    solve_one(near_one)
    acc_load.wait()
    for at in range(tiles):
        below_of(0, at)
    w_own(3, 2)
    w_y(3, 2)
    for at in range(len(plan[0][0]), len(order)):
        z_copies[at].wait_recv()
    off = off_near + off_one(far_one)
    v_far = v_near + v_one(far_one)
    for at in range(len(plan[1][1])):
        y_copies[len(y_copies) - 1 - at].wait_recv()
    partial[5] = off + off_one(shared)
    w_core(5, 1)
    vees[1, width:] = v_far + v_one(shared)
    found = vees[2] + thrice(
        tuple(piece[:size, :] for piece in right_one), split(vees[1]), (0, 0)
    )
    lefts[1] = found.reshape(lefts.shape[1:])
    lefts_out(1)
    w_last(0, 2)
    w_around(5)
    solve_one(far_one)
    solve_one(shared)
    lefts_away(1)
    w_y(2, 1)
    below_of(1, 0)
    below_of(1, 1)
    w_last(3, 2)
    for start in (0, 3):
        waits["own", start].wait_recv()
        waits["oth", start].wait_recv()

    inner = scale * (pre[0] - joined_at(0, 3))
    middle = split(inner + inner.T)
    cross_gram = thrice(split_two, split(joined_at(1, 4)), (0, 0))
    spread = thrice(
        split_two,
        split(
            thrice(
                middle, split(jnp.concatenate([inverse_two[...], crossed[...]], axis=1))
            )
        ),
        (0, 0),
    )
    sym_two[...] = spread[:, :size]
    half_two[...] = scale * spread[:, :size]
    following = split(grad_cross[...] - cross_gram - spread[:, size:])
    found = thrice(following, split_one)
    next_cross[...] = found
    cross_t[...] = found.T
    ready = pre[1] - (
        thrice(following, split_cross, (0, 0)) - thrice(split_cross, split(cross_gram), (0, 0))
    )
    w_gather(5)
    w_last(2, 1)
    below_of(1, 2)
    below_of(1, 3)
    mine_rows = pl.ds(pl.multiple_of(at_row * share, share), share)
    for copy in grad_left_loads:
        copy.wait()
    head = split(jnp.concatenate([sym_two[mine_rows, :], next_cross[mine_rows, :]], axis=1))
    grad_left[0] = (grad_left[0] - lefts_end(0)) - thrice(
        head, (left_high[...], left_low[...])
    )
    last = grad_left[1] - thrice(split(cross_t[mine_rows, :]), (left_high[:size], left_low[:size]))
    grad_left[1] = last - lefts_end(1)
    for start in (2, 5):
        waits["oth", start].wait_recv()
    waits["own", 5].wait_recv()
    inner = scale * (ready - joined_at(2, 5))
    middle_one[...] = inner + inner.T
    for copy in sends:
        copy.wait_send()


def tail_kernel(*refs):
    (
        acc,
        panel_out,
        half_two,
        next_cross,
        middle_one,
        inverse_one,
        grad_left,
        left_high,
        left_low,
    ) = refs[:9]
    (
        out_below,
        out_left_two,
        out_left_one,
        out_diag_two,
        out_diag_one,
        out_cross,
        out_panel_two,
        out_panel_one,
    ) = refs[9:17]
    sym_one, half_one, last, store_sem = refs[17:]
    size = sym_one.shape[0]
    share = last.shape[0]
    stores = []

    def store(source, target):
        copy = pltpu.make_async_copy(source, target, store_sem.at[len(stores)])
        copy.start()
        stores.append(copy)

    store(acc, out_below)
    store(panel_out.at[0], out_panel_two)
    store(panel_out.at[1], out_panel_one)
    store(half_two, out_diag_two)
    store(next_cross, out_cross)
    store(grad_left.at[0], out_left_two)
    inverse = split(inverse_one[...])
    found = thrice(inverse, split(thrice(split(middle_one[...]), inverse)), (0, 0))
    sym_one[...] = found
    rows, cols = grid_of(size)
    half_one[...] = jnp.where(rows > cols, found, jnp.where(rows == cols, 0.5 * found, 0.0))
    store(half_one, out_diag_one)
    mine_rows = pl.ds(pl.multiple_of(lax.axis_index("row") * share, share), share)
    last[...] = grad_left[1] - thrice(
        split(sym_one[mine_rows, :]), (left_high[size:, :], left_low[size:, :])
    )
    store(last, out_left_one)
    for copy in stores:
        copy.wait()


def invert_steps(blocks, events):
    size = blocks[0].shape[0]
    rows, cols = grid_of(size)
    apart = rows ^ cols
    lower = rows > cols
    inverses = []
    for block in blocks:
        diagonal = jnp.where(rows == cols, block, 0.0)
        down = 1.0 / jnp.sum(diagonal, axis=1, keepdims=True)
        across = 1.0 / jnp.sum(diagonal, axis=0, keepdims=True)
        pair = jnp.where(lower & (apart == 1), block, 0.0)
        inverses.append(jnp.where(rows == cols, down, 0.0) - pair * down * across)
    level = 1
    while (2 << level) <= size:
        mask = lower & ((apart >> level) == 1)
        steps = [
            small(jnp.where(mask, block, 0.0), inverse) for block, inverse in zip(blocks, inverses)
        ]
        inverses = [inverse - small(inverse, step) for inverse, step in zip(inverses, steps)]
        if level in events:
            events[level]()
        level += 1
    for late in sorted(events):
        if late >= level:
            events[late]()
    return inverses


def fused(*arrays):
    two, left, below, grad_left = arrays[0], arrays[3], arrays[5], arrays[11]
    size = two.shape[0]
    rows, width = arrays[14].shape
    columns = below.shape[1]
    share = grad_left.shape[0]
    quarter = width // 2
    piece = rows // 8
    plan = (
        ([piece // 2] * 8, []),
        ([piece // 2] * 6, [piece] * 2),
    )
    y_count = sum(len(go) + len(stay) for go, stay in plan)
    z_count = sum(len(go) for go, _ in plan)

    def real(*shape):
        return pltpu.VMEM(shape, jnp.float32)

    def short(*shape):
        return pltpu.VMEM(shape, jnp.bfloat16)

    def outs(*shape):
        return jax.ShapeDtypeStruct(shape, jnp.float32)

    scratch = [
        real(size, size),
        real(size, size),
        real(size, size),
        real(2 * size, columns),
        real(rows, columns),
        real(rows, size),
        real(size, size),
        real(size, size),
        real(size, size),
        real(rows, size),
        real(rows, size),
        short(rows, 2 * size),
        short(rows, 2 * size),
        real(3, size, columns),
        short(rows, columns),
        short(rows, columns),
        real(size, size),
        real(size, size),
        real(2, size, size),
        real(6, width, width),
        real(6, quarter, width),
        real(6, quarter, width),
        real(6, quarter, width),
        real(2, quarter, width),
        real(6, width, width),
        real(6, width, width),
        real(2, 2, 2, share, columns),
        real(2, 2, share, columns),
        real(2, share, columns),
        real(2, share, columns),
        real(size, size),
        real(size, size),
        pltpu.SemaphoreType.DMA((16,)),
        pltpu.SemaphoreType.DMA((y_count,)),
        pltpu.SemaphoreType.DMA((y_count,)),
        pltpu.SemaphoreType.DMA((z_count,)),
        pltpu.SemaphoreType.DMA((z_count,)),
        pltpu.SemaphoreType.DMA((18,)),
        pltpu.SemaphoreType.DMA((18,)),
        pltpu.SemaphoreType.DMA((6,)),
        pltpu.SemaphoreType.DMA((6,)),
    ]
    anywhere = pl.BlockSpec(memory_space=pl.ANY)
    near = pl.BlockSpec(memory_space=pltpu.VMEM)
    far = pl.BlockSpec(memory_space=pltpu.HBM)
    kept = pl.pallas_call(
        lambda *refs: fused_kernel(plan, *refs),
        out_shape=[
            real(rows, columns),
            real(2, rows, width),
            real(size, size),
            real(size, size),
            real(size, size),
            real(size, size),
            real(2, share, columns),
            short(2 * size, columns),
            short(2 * size, columns),
        ],
        in_specs=[far] * 16,
        out_specs=[near] * 9,
        scratch_shapes=scratch,
        compiler_params=pltpu.CompilerParams(
            collective_id=0,
            has_side_effects=True,
            vmem_limit_bytes=40 << 20,
        ),
        cost_estimate=pl.CostEstimate(
            flops=24 * rows * size * columns, bytes_accessed=16 * rows * columns, transcendentals=0
        ),
    )(*[pltpu.with_memory_space_constraint(values, pltpu.HBM) for values in arrays])
    return pl.pallas_call(
        tail_kernel,
        out_shape=[
            outs(rows, columns),
            outs(share, columns),
            outs(share, columns),
            outs(size, size),
            outs(size, size),
            outs(size, size),
            outs(rows, width),
            outs(rows, width),
        ],
        in_specs=[near] * 9,
        out_specs=[anywhere] * 8,
        scratch_shapes=[
            real(size, size),
            real(size, size),
            real(share, columns),
            pltpu.SemaphoreType.DMA((8,)),
        ],
        compiler_params=pltpu.CompilerParams(vmem_limit_bytes=8 << 20),
        cost_estimate=pl.CostEstimate(
            flops=12 * size**3, bytes_accessed=8 * rows * columns, transcendentals=0
        ),
    )(*[pltpu.with_memory_space_constraint(values, pltpu.VMEM) for values in kept])


def fits(mesh):
    return mesh.shape["row"] == 4 and mesh.shape["col"] == 2 and mesh.shape["depth"] % 2 == 0


def solution(mesh):
    panels = P("row", "col")
    lefts = P(None, ("col", "depth"))
    blocks = P("row", ("col", "depth"))
    return jax.shard_map(
        fused if fits(mesh) else body,
        mesh=mesh,
        in_specs=(P(), P(), P(), lefts, lefts, blocks, panels, panels)
        + (P(), P(), P(), blocks, blocks, blocks, panels, panels),
        out_specs=(blocks, blocks, blocks, P(), P(), P(), panels, panels),
        check_vma=False,
    )
```
